32 devices in a mesh: dom: 16 (over z, y, x), col: 2 (over core).
Axes of the slice: x: 2, y: 2, z: 4, core: 2. Of those that a mesh axis runs over, the one named last changes fastest.
Arguments:
- features: bfloat16 [16384, 256], P(('dom', 'col')), may hold values from -6 to 6
- weight: bfloat16 [256, 256], replicated, may hold values from -0.375 to 0.375
- cotangent: bfloat16 [16384, 256], P(('dom', 'col')), may hold values from -6 to 6
- tile_values: bfloat16 [1280, 128, 128], P(('dom', 'col')), may hold values from -0.15625 to 0.15625
- tile_rows: int32 [1280], P(('dom', 'col')), may hold values from 0 to 7
- tile_cols: int32 [1280], P(('dom', 'col')), may hold values from 0 to 19, as said below
- tile_count: int32 [32], P(('dom', 'col')), may hold values from 20 to 40, as said below
- send_blocks: int32 [32, 16], P(('dom', 'col')), may hold values from 0 to 3
Outputs:
- output_rows: bfloat16 [16384, 256], P(('dom', 'col'))
- feature_grad: bfloat16 [16384, 256], P(('dom', 'col'))
- weight_grad: float32 [256, 256], replicated
The draws below stay inside these ranges and needn't reach their ends.
Inputs may be any that keep to these rules, and one draw needn't show every extreme that they name: `tile_cols`: A value v below 4 names the device's own row block v; a value 4 + s names the row block that the device of partition s with the same col index sends to this partition; no receive slot is named by two tiles of one device. Only the first tile_count slots of a device's tiles are live; some device has all 40 live.
All inputs are finite; a program needn't handle non-finite values.
Results may differ from the reference program's by a relative error of at most 0.0049.
Values may be sent and summed in bfloat16 or wider, within the bound.
A program may use at most 128 MiB of HBM per device.

```python
import jax
import jax.numpy as jnp
from jax import lax

F_IN = 256
F_OUT = 256
BLK = 128
NB = 8
TILES = 40
NODES = 16384
N_DOM = 16
N_COL = 2


def draw_tile_cols(key, part):
    devices_all = N_DOM * N_COL
    half_blocks = NB // N_COL
    remote_count = min(N_DOM, 3 * TILES // 4)
    slot_keys = jax.random.split(jax.random.fold_in(key, 11), devices_all)
    slot_perms = jax.vmap(lambda k: jax.random.permutation(k, N_DOM))(slot_keys)
    remote = slot_perms[:, :remote_count] + half_blocks
    local_ids = jax.random.randint(jax.random.fold_in(key, 12), (devices_all, TILES - remote_count), 0, half_blocks)
    joined = jnp.concatenate([remote.astype(jnp.int32), local_ids.astype(jnp.int32)], axis=1)
    order_keys = jax.random.split(jax.random.fold_in(key, 13), devices_all)
    orders = jax.vmap(lambda k: jax.random.permutation(k, TILES))(order_keys)
    placed = jnp.take_along_axis(joined, orders.astype(jnp.int32), axis=1)
    return placed.reshape(devices_all * TILES).astype(jnp.int32)


def draw_tile_count(key, part):
    devices_all = N_DOM * N_COL
    base = jax.random.randint(jax.random.fold_in(key, 21), (devices_all,), 0, TILES)
    skewed = TILES // 2 + base * base // (2 * TILES)
    picked = jax.random.randint(jax.random.fold_in(key, 22), (), 0, devices_all)
    return jnp.where(jnp.arange(devices_all) == picked, TILES, skewed).astype(jnp.int32)


def set_ends(entries, own_key, least, high):
    longest = entries.shape.index(max(entries.shape))
    spots = []
    for shift in (0, 1):
        where = [jax.random.randint(jax.random.fold_in(own_key, axis), (), 0, length) for axis, length in enumerate(entries.shape)]
        where[longest] = (where[longest] + shift) % entries.shape[longest]
        spots.append(tuple(where))
    return entries.at[spots[0]].set(least).at[spots[1]].set(high)


def levels(stream_key, shape, cuts, low, top_value):
    gain = 1.0
    for axis_at, shards_of in cuts:
        heights = jax.random.uniform(jax.random.fold_in(jax.random.fold_in(stream_key, 6), axis_at), (shards_of,), jnp.float32, low / len(cuts), top_value / len(cuts))
        gain = gain * jnp.repeat(jnp.exp(heights), shape[axis_at] // shards_of).reshape((-1,) + (1,) * (len(shape) - 1 - axis_at))
    return gain


def bell_draw(key, shape, scale, reach, cuts=(), held_as=jnp.bfloat16):
    array = jax.random.normal(key, shape, jnp.float32) * scale
    if len(cuts) > 0:
        array = levels(key, shape, cuts, -0.22, 0.18) * array
    return jnp.clip(array, min=-reach, max=reach).astype(held_as)


def setup_inputs(seed: int = 0) -> dict:
    key_list = jax.random.split(jax.random.key(seed), 9)
    features = bell_draw(key_list[0], (NODES, F_IN), 1.0, 6.0, ((0, 32),))
    weight = bell_draw(key_list[1], (F_IN, F_OUT), F_IN ** -0.5, 0.375)
    cotangent = bell_draw(key_list[2], (NODES, F_OUT), 1.0, 6.0, ((0, 32),))
    tile_values = bell_draw(key_list[3], (N_DOM * N_COL * TILES, BLK, BLK), (10 * BLK) ** -0.5, 0.15625, ((0, 32),))
    tile_rows = set_ends(jax.random.randint(key_list[4], (N_DOM * N_COL * TILES,), 0, NB), jax.random.fold_in(key_list[4], 1), 0, NB - 1).astype(jnp.int32)
    tile_cols = draw_tile_cols(jax.random.fold_in(key_list[8], 71), 0)
    tile_count = draw_tile_count(jax.random.fold_in(key_list[8], 71), 0)
    send_blocks = set_ends(jax.random.randint(key_list[7], (N_DOM * N_COL, N_DOM), 0, NB // N_COL), jax.random.fold_in(key_list[7], 1), 0, (NB // N_COL) - 1).astype(jnp.int32)
    return dict(features=features, weight=weight, cotangent=cotangent, tile_values=tile_values, tile_rows=tile_rows, tile_cols=tile_cols, tile_count=tile_count, send_blocks=send_blocks)


def reference(features, weight, cotangent, tile_values, tile_rows, tile_cols, tile_count, send_blocks):
    devices_all = N_DOM * N_COL
    half_blocks = NB // N_COL
    total_blocks = NB * N_DOM
    blocks = features.reshape(total_blocks, BLK, F_IN)
    tiles = tile_values.reshape(devices_all, TILES, BLK, BLK)
    rows_local = tile_rows.reshape(devices_all, TILES).astype(jnp.int32)
    cols_local = tile_cols.reshape(devices_all, TILES).astype(jnp.int32)
    device_ids = jnp.arange(devices_all, dtype=jnp.int32)
    part_ids = (device_ids // N_COL)[:, None]
    core_ids = (device_ids % N_COL)[:, None]
    slots = jnp.clip(cols_local - half_blocks, 0, N_DOM - 1).astype(jnp.int32)
    sender = (slots * N_COL + core_ids).astype(jnp.int32)
    sent_ids = send_blocks.astype(jnp.int32)[sender, jnp.broadcast_to(part_ids, sender.shape)]
    remote_block = slots * NB + core_ids * half_blocks + sent_ids
    own_block = part_ids * NB + core_ids * half_blocks + cols_local
    global_cols = jnp.where(cols_local < half_blocks, own_block, remote_block).astype(jnp.int32)
    global_rows = (part_ids * NB + rows_local).astype(jnp.int32)
    live_mask = (jnp.arange(TILES, dtype=jnp.int32)[None, :] < tile_count.astype(jnp.int32)[:, None]).astype(jnp.float32)

    def forward_step(carry, inputs):
        tile_block, live_row, row_ids, col_ids = inputs
        weighted = tile_block.astype(jnp.float32) * live_row[:, None, None]
        picked = blocks[col_ids].astype(jnp.float32)
        terms = jnp.einsum("tij,tjf->tif", weighted, picked, precision=lax.Precision.HIGHEST)
        return carry.at[row_ids].add(terms), None

    hidden_sum, _ = lax.scan(forward_step, jnp.zeros((total_blocks, BLK, F_IN), jnp.float32),
                             (tiles, live_mask, global_rows, global_cols))
    hidden = hidden_sum.astype(jnp.bfloat16).reshape(NODES, F_IN)
    output_rows = jnp.dot(hidden, weight, preferred_element_type=jnp.float32).astype(jnp.bfloat16)
    grad_hidden = lax.dot_general(cotangent, weight, (((1,), (1,)), ((), ())),
                                  preferred_element_type=jnp.float32).astype(jnp.bfloat16)
    grad_blocks = grad_hidden.reshape(total_blocks, BLK, F_IN)

    def backward_step(carry, inputs):
        tile_block, live_row, row_ids, col_ids = inputs
        weighted = tile_block.astype(jnp.float32) * live_row[:, None, None]
        picked = grad_blocks[row_ids].astype(jnp.float32)
        terms = jnp.einsum("tji,tjf->tif", weighted, picked, precision=lax.Precision.HIGHEST)
        return carry.at[col_ids].add(terms), None

    grad_sum, _ = lax.scan(backward_step, jnp.zeros((total_blocks, BLK, F_IN), jnp.float32),
                           (tiles, live_mask, global_rows, global_cols))
    feature_grad = grad_sum.astype(jnp.bfloat16).reshape(NODES, F_IN)
    weight_grad = lax.dot_general(hidden, cotangent, (((0,), (0,)), ((), ())),
                                  preferred_element_type=jnp.float32)
    weight_grad = weight_grad * jnp.float32(1.0 / (NODES ** 0.5))
    return output_rows, feature_grad, weight_grad
```

```python
import functools

import jax
import jax.numpy as jnp
from jax import lax
from jax.experimental import pallas as pl
from jax.experimental.pallas import tpu as pltpu
from jax.sharding import PartitionSpec as P

MESH = pl.DeviceIdType.MESH
F32 = jnp.float32
BF16 = jnp.bfloat16
Q = 4


def kernel(scale, rows_s, cols_s, count_s, send_s, feat_hbm, weight_hbm, cot_hbm, tiles_hbm,
           out, fgrad, wgrad,
           feat, weight, cot, tiles, sendf, recvf, sendb, recvb, gin, buf, base, gh, psend, precv, hid,
           wsend, wrecv, wchunk, wpart, wall, wpeer, tos, table, *rest):
    lines = rest[:2 * (Q - 1)]
    (t_send, t_recv, lf_send, lf_recv, s_send, s_recv, pf_send, pf_recv, pb_send, pb_recv,
     r_send, r_recv, g_send, g_recv, misc) = rest[2 * (Q - 1):]
    slots = tiles.shape[0]
    half, blk, width = feat.shape
    plane = recvf.shape[1]
    n = Q * plane
    blocks = 2 * half
    top = Q - 1
    me = lax.axis_index("dom")
    col = lax.axis_index("col")
    other = 1 - col
    count = count_s[0]
    z, w = lax.div(me, plane), lax.rem(me, plane)
    below = (z, top - z)

    side = n // 2
    mine_side, spot = lax.div(me, side), lax.rem(me, side)

    def peer_side(k):
        return lax.rem(mine_side + 1 + lax.div(k - 1, side), 2) * side

    def to_peer(k):
        return peer_side(k) + lax.rem(spot + k, side)

    def from_peer(k):
        return peer_side(k) + lax.rem(spot + 2 * side - k, side)

    def remote(src, dst, s_sem, r_sem, dom, core):
        return pltpu.make_async_remote_copy(
            src_ref=src, dst_ref=dst, send_sem=s_sem, recv_sem=r_sem,
            device_id=(dom, core), device_id_type=MESH)

    feat_copy = pltpu.make_async_copy(feat_hbm, feat, misc.at[9])
    feat_copy.start()
    cot_copy = pltpu.make_async_copy(cot_hbm, cot, misc.at[10])
    cot_copy.start()
    weight_copy = pltpu.make_async_copy(weight_hbm, weight, misc.at[11])
    weight_copy.start()
    tile_copy = pltpu.make_async_copy(tiles_hbm, tiles, misc.at[0])
    tile_copy.start()

    barrier = pltpu.get_barrier_semaphore()

    def greet(k, carry):
        pl.semaphore_signal(barrier, inc=1, device_id=(to_peer(k), col), device_id_type=MESH)
        return carry

    lax.fori_loop(1, n, greet, 0)
    pl.semaphore_signal(barrier, inc=1, device_id=(me, other), device_id_type=MESH)

    gin[...] = jnp.zeros(gin.shape, gin.dtype)
    buf[0] = jnp.zeros((blk, width), F32)

    def keep(i, carry):
        table[z, i] = send_s[i]
        return carry

    lax.fori_loop(0, n, keep, 0)

    def pf_copy(s, peer, slot):
        return remote(sendf.at[s, peer], recvf.at[s, slot], pf_send.at[s, peer], pf_recv.at[s, slot],
                      z * plane + peer, col)

    def pb_copy(s, peer, slot):
        return remote(sendb.at[s, peer], recvb.at[s, slot], pb_send.at[s, peer], pb_recv.at[s, slot],
                      z * plane + peer, col)

    def peers(body):
        def step(k, carry):
            body(lax.rem(w + k, plane))
            return carry

        lax.fori_loop(1, plane, step, 0)

    def pick(source, s):
        def one(peer):
            sendf[s, peer] = source[table[s, z * plane + peer]]

        peers(one)
        recvf[s, w] = source[table[s, me]]

    def spread(s):
        peers(lambda peer: pf_copy(s, peer, w).start())

    feat_copy.wait()
    pick(feat, z)

    cot_copy.wait()
    weight_copy.wait()
    own = lax.dot_general(cot[...], weight[...], (((1,), (1,)), ((), ())),
                          preferred_element_type=F32).astype(BF16)
    gh[pl.ds(col * half, half)] = own.reshape(half, blk, width)

    def find(s, carry):
        found = jnp.int32(0)
        for t in range(slots):
            found = jnp.where((cols_s[t] == s + half) & (t < count), t + 1, found)
        tos[s] = found
        return carry

    lax.fori_loop(0, n, find, 0)

    pl.semaphore_wait(barrier, n)

    def held(d, k):
        return feat if k == 0 else lines[d * top + k - 1]

    def lf_copy(d, k, j):
        nxt = z + 1 if d == 0 else z - 1
        return remote(held(d, k).at[j], held(d, k + 1).at[j], lf_send.at[d, k, j], lf_recv.at[d, k, j],
                      nxt * plane + w, col)

    def s_copy(d, s, j):
        nxt = z + 1 if d == 0 else z - 1
        slot = s if d == 0 else jnp.where(s == nxt, Q, s)
        return remote(gin.at[s, j], gin.at[slot, j], s_send.at[s, j], s_recv.at[slot, j],
                      nxt * plane + w, col)

    def line(k):
        return lax.rem(z + k, Q)

    def t_copy(k, slot):
        return remote(send_s, table.at[slot], t_send.at[k], t_recv.at[slot], line(k) * plane + w, col)

    for j in range(half):
        for d in range(2):
            @pl.when(below[d] < top)
            def _():
                lf_copy(d, 0, j).start()

    for k in range(1, Q):
        t_copy(k, z).start()
    spread(z)

    gh_half = gh.at[pl.ds(col * half, half)]
    gh_copy = remote(gh_half, gh_half, misc.at[1], misc.at[2], me, other)
    gh_copy.start()

    tile_copy.wait()
    gh_copy.wait_send()
    gh_other = gh.at[pl.ds(other * half, half)]
    remote(gh_other, gh_other, misc.at[1], misc.at[2], me, other).wait_recv()

    def back_term(slot):
        found = tos[slot]
        at = jnp.maximum(found - 1, 0)
        term = lax.dot_general(tiles[at], gh[rows_s[at]], (((0,), (0,)), ((), ())),
                               preferred_element_type=F32)
        return jnp.where(found > 0, term, 0.0).astype(BF16)

    low_side = lax.div(z, Q // 2)
    far = top * (1 - low_side)
    near = 2 - low_side
    pair = z + 1 - 2 * lax.rem(z, 2)
    for s in (far, near, pair, z):
        def fill(k, carry, s=s):
            peer = lax.rem(w + k, plane)
            sendb[s, peer] = back_term(s * plane + peer)
            return carry

        lax.fori_loop(0, plane, fill, 0, unroll=4)
        recvb[s, w] = sendb[s, w]
        peers(lambda peer, s=s: pb_copy(s, peer, w).start())

    def link(lasts, key, index):
        prev = jnp.int32(0)
        for r, last in enumerate(lasts):
            prev = jnp.where(key == r, last, prev)
        return prev, tuple(jnp.where(key == r, index, last) for r, last in enumerate(lasts))

    def own_back(t, lasts):
        key = jnp.where(t < count, cols_s[t], -1)
        prev, lasts = link(lasts, key, t + 1)
        term = lax.dot_general(tiles[t], gh[rows_s[t]], (((0,), (0,)), ((), ())),
                               preferred_element_type=F32)
        buf[t + 1] = buf[prev] + term
        return lasts

    unroll = 4 if slots % 4 == 0 else 1
    lasts = lax.fori_loop(0, slots, own_back, (jnp.int32(0),) * half, unroll=unroll)
    for j in range(half):
        base[j] = buf[lasts[j]]

    def own_fwd(t, lasts):
        source = cols_s[t]
        key = jnp.where((t < count) & (source < half), rows_s[t], -1)
        prev, lasts = link(lasts, key, t + 1)
        term = jnp.dot(tiles[t], feat[jnp.minimum(source, half - 1)], preferred_element_type=F32)
        buf[t + 1] = buf[prev] + term
        return lasts

    def slot_group(g, lasts):
        if g == 0:
            s = z
        else:
            zm = z + low_side * (top - 2 * z)
            rel = g - 1 + jnp.where(g <= zm, 0, 1)
            s = rel + low_side * (top - 2 * rel)
        peers(lambda peer: pf_copy(s, peer, peer).wait_recv())

        def step(k, lasts):
            slot = lax.rem(w + k, plane)
            found = tos[s * plane + slot]
            at = jnp.maximum(found - 1, 0)
            key = jnp.where(found > 0, rows_s[at], -1)
            index = slots + 1 + g * plane + k
            prev, lasts = link(lasts, key, index)
            term = jnp.dot(tiles[at], recvf[s, slot], preferred_element_type=F32)
            buf[index] = buf[prev] + term
            return lasts

        return lax.fori_loop(0, plane, step, lasts, unroll=4)

    span = 64

    def add_terms(s, j):
        def rows(i, carry):
            at = pl.ds(pl.multiple_of(i * span, span), span)

            def add(slot, acc):
                value = recvb[s, slot, at, :].astype(F32)
                return acc + jnp.where(table[s, z * plane + slot] == j, value, 0.0)

            acc = lax.fori_loop(0, plane, add, gin[s, j, at, :].astype(F32), unroll=4)
            gin[s, j, at, :] = acc.astype(BF16)
            return carry

        lax.fori_loop(0, blk // span, rows, 0)

    def sum_of(k, d):
        rel = top - (k - below[d])
        return rel if d == 0 else top - rel

    def feat_of(k, d):
        rel = below[d] - 1 - k
        return rel if d == 0 else top - rel

    def line_step(k):
        for d in range(2):
            @pl.when(below[d] <= k)
            def _():
                peers(lambda peer: pb_copy(sum_of(k, d), peer, peer).wait_recv())

        def chunk(j, carry):
            for d in range(2):
                @pl.when(k < below[d])
                def _():
                    lf_copy(d, k, j).wait_recv()

                    if k + 1 < top:
                        @pl.when(below[d] < top)
                        def _():
                            lf_copy(d, k + 1, j).start()

            for d in range(2):
                @pl.when(below[d] <= k)
                def _():
                    s = sum_of(k, d)

                    @pl.when(below[d] > 0)
                    def _():
                        remote(gin.at[s, j], gin.at[s, j], s_send.at[s, j], s_recv.at[s, j], me, other).wait_recv()

                    add_terms(s, j)
                    s_copy(d, s, j).start()
            return carry

        lax.fori_loop(0, half, chunk, 0)
        for d in range(2):
            @pl.when(k < below[d])
            def _():
                pick(held(d, k + 1), feat_of(k, d))
                spread(feat_of(k, d))

    for k in range(1, Q):
        t_copy(k, line(k)).wait_recv()

    line_step(0)
    lasts = lax.fori_loop(0, slots, own_fwd, (jnp.int32(0),) * blocks, unroll=unroll)
    lasts = slot_group(0, lasts)
    for k in range(1, Q - 1):
        line_step(k)
        lasts = slot_group(k, lasts)
    lasts = slot_group(Q - 1, lasts)

    for j in range(half):
        psend[j] = buf[jnp.where(col == 0, lasts[half + j], lasts[j])]
    p_copy = remote(psend, precv, misc.at[3], misc.at[4], me, other)
    p_copy.start()
    p_copy.wait()
    for j in range(half):
        mine = buf[jnp.where(col == 0, lasts[j], lasts[half + j])]
        hid[pl.ds(j * blk, blk), :] = (mine + precv[j]).astype(jnp.bfloat16)

    local = lax.dot_general(hid[...], cot[...], (((0,), (0,)), ((), ())),
                            preferred_element_type=F32) * jnp.float32(scale)
    wh = width // 2
    low, high = local[:wh], local[wh:]
    wsend[...] = jnp.where(col == 0, high, low)
    w_copy = remote(wsend, wrecv, misc.at[5], misc.at[6], me, other)
    w_copy.start()
    out[...] = jnp.dot(hid[...], weight[...], preferred_element_type=F32).astype(jnp.bfloat16)
    w_copy.wait()
    share = jnp.where(col == 0, low, high) + wrecv[...]
    wchunk[...] = share.reshape(wchunk.shape)

    def r_copy(peer, chunk, slot):
        return remote(wchunk.at[chunk], wpart.at[slot], r_send.at[chunk], r_recv.at[slot], peer, col)

    def r_start(k, carry):
        r_copy(to_peer(k), to_peer(k), me).start()
        return carry

    lax.fori_loop(1, n, r_start, 0)
    wpart[me] = wchunk[me]

    def r_wait(k, carry):
        r_copy(from_peer(k), from_peer(k), from_peer(k)).wait_recv()
        return carry

    lax.fori_loop(1, n, r_wait, 0)
    wall[me] = jnp.sum(wpart[...], axis=0)

    def g_copy(k, peer, slot):
        return remote(wall.at[slot], wall.at[slot], g_send.at[k], g_recv.at[slot], peer, col)

    def g_start(k, carry):
        g_copy(k, to_peer(k), me).start()
        return carry

    lax.fori_loop(1, n, g_start, 0)

    def g_wait(k, carry):
        g_copy(k, from_peer(k), from_peer(k)).wait_recv()
        return carry

    lax.fori_loop(1, n, g_wait, 0)
    x_copy = remote(wall, wpeer, misc.at[7], misc.at[8], me, other)
    x_copy.start()
    wgrad[pl.ds(pl.multiple_of(col * wh, wh), wh), :] = wall[...].reshape(wh, wgrad.shape[1])

    peers(lambda peer: pb_copy(z, peer, peer).wait_recv())

    def sums_in(j, carry):
        for d in range(2):
            @pl.when(below[d] > 0)
            def _():
                slot = z if d == 0 else Q
                remote(gin.at[slot, j], gin.at[slot, j], s_send.at[z, j], s_recv.at[slot, j], me, other).wait_recv()
        return carry

    lax.fori_loop(0, half, sums_in, 0)
    step = 16

    def total(i, carry):
        at = pl.ds(pl.multiple_of(i * step, step), step)

        def add(slot, sums):
            value = recvb[z, slot, at, :].astype(F32)
            home = send_s[z * plane + slot]
            return tuple(acc + jnp.where(home == j, value, 0.0) for j, acc in enumerate(sums))

        start = tuple(base[j, at, :] + gin[z, j, at, :].astype(F32) + gin[Q, j, at, :].astype(F32)
                      for j in range(half))
        sums = lax.fori_loop(0, plane, add, start, unroll=4)
        for j in range(half):
            fgrad[j, at, :] = sums[j].astype(BF16)
        return carry

    lax.fori_loop(0, blk // step, total, 0)

    for k in range(1, Q):
        t_copy(k, z).wait_send()
    for s in range(Q):
        def sent(peer, s=s):
            pf_copy(s, peer, w).wait_send()
            pb_copy(s, peer, w).wait_send()

        peers(sent)

    def line_sent(j, carry):
        for d in range(2):
            for k in range(Q - 1):
                @pl.when((k <= below[d]) & (below[d] < top))
                def _():
                    lf_copy(d, k, j).wait_send()
            for k in range(Q - 1):
                @pl.when(below[d] <= k)
                def _():
                    s_copy(d, sum_of(k, d), j).wait_send()
        return carry

    lax.fori_loop(0, half, line_sent, 0)

    def drain(k, carry):
        r_copy(to_peer(k), to_peer(k), me).wait_send()
        g_copy(k, to_peer(k), me).wait_send()
        return carry

    lax.fori_loop(1, n, drain, 0)
    x_copy.wait()
    wgrad[pl.ds(pl.multiple_of(other * wh, wh), wh), :] = wpeer[...].reshape(wh, wgrad.shape[1])


def place(*refs):
    count = (len(refs) - 1) // 3
    sources, targets, held, sem = refs[:count], refs[count:2 * count], refs[2 * count:-1], refs[-1]
    reads = [pltpu.make_async_copy(a, h, sem.at[i]) for i, (a, h) in enumerate(zip(sources, held))]
    writes = [pltpu.make_async_copy(h, b, sem.at[count + i]) for i, (h, b) in enumerate(zip(held, targets))]
    for read in reads:
        read.start()
    for read, write in zip(reads, writes):
        read.wait()
        write.start()
    for write in writes:
        write.wait()


def finish(*arrays):
    hbm = pl.BlockSpec(memory_space=pl.ANY)
    return pl.pallas_call(
        place,
        out_shape=tuple(jax.ShapeDtypeStruct(a.shape, a.dtype) for a in arrays),
        in_specs=[hbm] * len(arrays),
        out_specs=(hbm,) * len(arrays),
        scratch_shapes=[pltpu.VMEM(a.shape, a.dtype) for a in arrays]
        + [pltpu.SemaphoreType.DMA((2 * len(arrays),))],
    )(*arrays)


def local(features, weight, cotangent, tile_values, tile_rows, tile_cols, tile_count, send_blocks):
    slots, blk, _ = tile_values.shape
    rows, width = features.shape
    width_out = cotangent.shape[1]
    half = rows // blk
    n = send_blocks.shape[1]
    plane = n // Q
    nodes = rows * lax.axis_size("col") * lax.axis_size("dom")
    scale = 1.0 / nodes**0.5
    bf = jnp.bfloat16
    chunk = width // 2 // n
    vmem = pl.BlockSpec(memory_space=pltpu.VMEM)
    hbm = pl.BlockSpec(memory_space=pl.ANY)
    smem = pl.BlockSpec(memory_space=pltpu.SMEM)
    sems = pltpu.SemaphoreType.DMA
    out, fgrad, wgrad = pl.pallas_call(
        functools.partial(kernel, scale),
        out_shape=(
            jax.ShapeDtypeStruct((rows, width_out), bf),
            jax.ShapeDtypeStruct((half, blk, width), bf),
            jax.ShapeDtypeStruct((width, width_out), F32),
        ),
        in_specs=[smem] * 4 + [hbm] * 4,
        out_specs=(vmem, vmem, vmem),
        scratch_shapes=[
            pltpu.VMEM((half, blk, width), bf),
            pltpu.VMEM((width, width_out), bf),
            pltpu.VMEM((rows, width_out), bf),
            pltpu.VMEM((slots, blk, blk), bf),
            pltpu.VMEM((Q, plane, blk, width), bf),
            pltpu.VMEM((Q, plane, blk, width), bf),
            pltpu.VMEM((Q, plane, blk, width), bf),
            pltpu.VMEM((Q, plane, blk, width), bf),
            pltpu.VMEM((Q + 1, half, blk, width), bf),
            pltpu.VMEM((slots + 1 + n, blk, width), F32),
            pltpu.VMEM((half, blk, width), F32),
            pltpu.VMEM((2 * half, blk, width), bf),
            pltpu.VMEM((half, blk, width), F32),
            pltpu.VMEM((half, blk, width), F32),
            pltpu.VMEM((rows, width), bf),
            pltpu.VMEM((width // 2, width_out), F32),
            pltpu.VMEM((width // 2, width_out), F32),
            pltpu.VMEM((n, chunk, width_out), F32),
            pltpu.VMEM((n, chunk, width_out), F32),
            pltpu.VMEM((n, chunk, width_out), F32),
            pltpu.VMEM((n, chunk, width_out), F32),
            pltpu.SMEM((n,), jnp.int32),
            pltpu.SMEM((Q, n), jnp.int32),
        ] + [pltpu.VMEM((half, blk, width), bf)] * (2 * (Q - 1)) + [
            sems((Q,)), sems((Q,)),
            sems((2, Q - 1, half)), sems((2, Q - 1, half)),
            sems((Q, half)), sems((Q + 1, half)),
        ] + [sems((Q, plane))] * 4 + [sems((n,))] * 4 + [sems((12,))],
        compiler_params=pltpu.CompilerParams(
            collective_id=0, has_side_effects=True, vmem_limit_bytes=67000000),
    )(tile_rows, tile_cols, tile_count, send_blocks.reshape(n),
      features.reshape(half, blk, width), weight, cotangent, tile_values)
    return finish(out, fgrad.reshape(rows, width), wgrad)


def solution(mesh):
    return jax.shard_map(
        local,
        mesh=mesh,
        in_specs=(
            P(("dom", "col"), None),
            P(),
            P(("dom", "col"), None),
            P(("dom", "col"), None, None),
            P(("dom", "col")),
            P(("dom", "col")),
            P(("dom", "col")),
            P(("dom", "col"), None),
        ),
        out_specs=(P(("dom", "col"), None), P(("dom", "col"), None), P()),
        check_vma=False,
    )
```

```python
import functools

import jax
import jax.numpy as jnp
from jax import lax
from jax.experimental import pallas as pl
from jax.experimental.pallas import tpu as pltpu
from jax.sharding import PartitionSpec as P

MESH = pl.DeviceIdType.MESH
F32 = jnp.float32
BF16 = jnp.bfloat16
Q = 4
CH = 4


def kernel(scale, owners, rows_s, cols_s, count_s, send_s, feat_hbm, weight_hbm, cot_hbm, tiles_hbm,
           out_hbm, fgrad_hbm, wgrad_hbm,
           feat, weight, cot, tiles, sendf, recvf, sendb, recvb, gin, buf, base, gh, psend, precv, hid,
           part, out, fgrad, wgrad, wchunk, wpart, wall, tos, table, *rest):
    lines = rest[:2 * (Q - 1) * CH]
    (t_send, t_recv, lf_send, lf_recv, s_send, s_recv, pf_send, pf_recv, pb_send, pb_recv,
     r_send, r_recv, g_send, g_recv, misc) = rest[2 * (Q - 1) * CH:]
    slots = tiles.shape[0]
    half, blk, width = feat.shape
    plane = recvf.shape[1]
    n = Q * plane
    blocks = 2 * half
    top = Q - 1
    tall = blk // CH
    me = lax.axis_index("dom")
    col = lax.axis_index("col")
    other = 1 - col
    count = count_s[0]
    z, w = lax.div(me, plane), lax.rem(me, plane)
    below = (z, top - z)
    flat = 2 * me + col

    def remote(src, dst, s_sem, r_sem, dom, core):
        return pltpu.make_async_remote_copy(
            src_ref=src, dst_ref=dst, send_sem=s_sem, recv_sem=r_sem,
            device_id=(dom, core), device_id_type=MESH)

    def line(k):
        return lax.rem(z + k, Q)

    def peers(body):
        def step(k, carry):
            body(lax.rem(w + k, plane))
            return carry

        lax.fori_loop(1, plane, step, 0)

    feat_copy = pltpu.make_async_copy(feat_hbm, feat, misc.at[0])
    feat_copy.start()
    barrier = pltpu.get_barrier_semaphore()

    def greet(dom, core):
        pl.semaphore_signal(barrier, inc=1, device_id=(dom, core), device_id_type=MESH)

    for k in range(1, Q):
        greet(line(k) * plane + w, col)
    peers(lambda peer: greet(z * plane + peer, col))
    greet(me, other)
    rows = half * blk
    cot_half = cot.at[pl.ds(pl.multiple_of(col * rows, rows), rows)]
    cot_copy = pltpu.make_async_copy(cot_hbm, cot_half, misc.at[1])
    cot_copy.start()
    weight_copy = pltpu.make_async_copy(weight_hbm, weight, misc.at[2])
    weight_copy.start()
    tile_copy = pltpu.make_async_copy(tiles_hbm, tiles, misc.at[3])
    tile_copy.start()

    gin[...] = jnp.zeros(gin.shape, gin.dtype)
    buf[0] = jnp.zeros((blk, width), F32)

    def keep(i, carry):
        table[z, i] = send_s[i]
        return carry

    lax.fori_loop(0, n, keep, 0)

    def part_of(c):
        return pl.ds(c * tall, tall)

    def pf_copy(s, peer, slot, at):
        return remote(sendf.at[s, peer, at], recvf.at[s, slot, at], pf_send.at[s, peer], pf_recv.at[s, slot],
                      z * plane + peer, col)

    def pb_copy(s, peer, slot):
        return remote(sendb.at[s, peer], recvb.at[s, slot], pb_send.at[s, peer], pb_recv.at[s, slot],
                      z * plane + peer, col)

    whole = pl.ds(0, blk)

    def spread(source, s, at):
        def one(peer):
            sendf[s, peer, at, :] = source[table[s, z * plane + peer]]

        peers(one)
        peers(lambda peer: pf_copy(s, peer, w, at).start())
        recvf[s, w, at, :] = source[table[s, me]]

    def lf_copy(d, k, c):
        nxt = z + 1 if d == 0 else z - 1
        src = feat.at[:, part_of(c)] if k == 0 else lines[(d * top + k - 1) * CH + c]
        return remote(src, lines[(d * top + k) * CH + c], lf_send.at[d, k, c], lf_recv.at[d, k, c],
                      nxt * plane + w, col)

    def s_copy(d, s, c):
        nxt = z + 1 if d == 0 else z - 1
        slot = s if d == 0 else jnp.where(s == nxt, Q, s)
        return remote(gin.at[s, :, part_of(c)], gin.at[slot, :, part_of(c)], s_send.at[s, c], s_recv.at[slot, c],
                      nxt * plane + w, col)

    def s_wait(slot, c):
        remote(gin.at[slot, :, part_of(c)], gin.at[slot, :, part_of(c)], s_send.at[0, c], s_recv.at[slot, c],
               me, other).wait_recv()

    def t_copy(k, slot):
        return remote(send_s, table.at[slot], t_send.at[k], t_recv.at[slot], line(k) * plane + w, col)

    feat_copy.wait()
    pl.semaphore_wait(barrier, top + plane)

    for k in range(1, Q):
        t_copy(k, z).start()
    for c in range(CH):
        for d in range(2):
            @pl.when(below[d] < top)
            def _():
                lf_copy(d, 0, c).start()

    spread(feat, z, whole)
    cot_copy.wait()
    c_copy = remote(cot_half, cot_half, misc.at[4], misc.at[5], me, other)
    c_copy.start()

    def find(s, carry):
        found = jnp.int32(0)
        for t in range(slots):
            found = jnp.where((cols_s[t] == s + half) & (t < count), t + 1, found)
        tos[s] = found
        return carry

    lax.fori_loop(0, n, find, 0)
    weight_copy.wait()
    cot_other = cot.at[pl.ds(pl.multiple_of(other * rows, rows), rows)]
    remote(cot_other, cot_other, misc.at[4], misc.at[5], me, other).wait_recv()
    gh[...] = lax.dot_general(cot[...], weight[...], (((1,), (1,)), ((), ())),
                              preferred_element_type=F32).astype(BF16).reshape(gh.shape)
    tile_copy.wait()

    def back_term(slot):
        found = tos[slot]
        at = jnp.maximum(found - 1, 0)
        term = lax.dot_general(tiles[at], gh[rows_s[at]], (((0,), (0,)), ((), ())),
                               preferred_element_type=F32)
        return jnp.where(found > 0, term, 0.0).astype(BF16)

    def back_send(s):
        peers(lambda peer: pb_copy(s, peer, w).start())

    low_side = lax.div(z, Q // 2)
    far = top * (1 - low_side)
    near = 2 - low_side
    pair = z + 1 - 2 * lax.rem(z, 2)
    for i, s in enumerate((far, near, pair, z)):
        def fill(k, carry, s=s):
            peer = lax.rem(w + k, plane)
            sendb[s, peer] = back_term(s * plane + peer)
            return carry

        lax.fori_loop(0, plane, fill, 0, unroll=4)
        recvb[s, w] = sendb[s, w]
        if i < top:
            back_send(s)

    def link(lasts, key, index):
        prev = jnp.int32(0)
        for r, last in enumerate(lasts):
            prev = jnp.where(key == r, last, prev)
        return prev, tuple(jnp.where(key == r, index, last) for r, last in enumerate(lasts))

    def own_back(t, lasts):
        key = jnp.where(t < count, cols_s[t], -1)
        prev, lasts = link(lasts, key, t + 1)
        term = lax.dot_general(tiles[t], gh[rows_s[t]], (((0,), (0,)), ((), ())),
                               preferred_element_type=F32)
        buf[t + 1] = buf[prev] + term
        return lasts

    unroll = 4 if slots % 4 == 0 else 1

    def own_fwd(t, lasts):
        source = cols_s[t]
        key = jnp.where((t < count) & (source < half), rows_s[t], -1)
        prev, lasts = link(lasts, key, t + 1)
        term = jnp.dot(tiles[t], feat[jnp.minimum(source, half - 1)], preferred_element_type=F32)
        buf[t + 1] = buf[prev] + term
        return lasts

    def slot_group(g, lasts):
        if g == 0:
            s = z
        else:
            zm = z + low_side * (top - 2 * z)
            rel = g - 1 + jnp.where(g <= zm, 0, 1)
            s = rel + low_side * (top - 2 * rel)
        peers(lambda peer: pf_copy(s, peer, peer, whole).wait_recv())

        def step(k, lasts):
            slot = lax.rem(w + k, plane)
            found = tos[s * plane + slot]
            at = jnp.maximum(found - 1, 0)
            key = jnp.where(found > 0, rows_s[at], -1)
            index = slots + 1 + g * plane + k
            prev, lasts = link(lasts, key, index)
            term = jnp.dot(tiles[at], recvf[s, slot], preferred_element_type=F32)
            buf[index] = buf[prev] + term
            return lasts

        return lax.fori_loop(0, plane, step, lasts, unroll=4)

    def sums(s, at, starts):
        def add(slot, accs):
            value = recvb[s, slot, at, :].astype(F32)
            home = table[s, z * plane + slot]
            return tuple(acc + jnp.where(home == j, value, 0.0) for j, acc in enumerate(accs))

        return lax.fori_loop(0, plane, add, starts, unroll=4)

    def sum_of(k, d):
        rel = top - (k - below[d])
        return rel if d == 0 else top - rel

    def feat_of(k, d):
        rel = below[d] - 1 - k
        return rel if d == 0 else top - rel

    def feats(k):
        for c in range(CH):
            for d in range(2):
                @pl.when(k < below[d])
                def _():
                    lf_copy(d, k, c).wait_recv()

                    if k + 1 < top:
                        @pl.when(below[d] < top)
                        def _():
                            lf_copy(d, k + 1, c).start()

            for d in range(2):
                @pl.when(k < below[d])
                def _():
                    spread(lines[(d * top + k) * CH + c], feat_of(k, d), part_of(c))

    def grads(k):
        for d in range(2):
            @pl.when(below[d] <= k)
            def _():
                peers(lambda peer: pb_copy(sum_of(k, d), peer, peer).wait_recv())

        step = tall // 2
        for c in range(CH):
            for d in range(2):
                @pl.when(below[d] <= k)
                def _():
                    s = sum_of(k, d)

                    @pl.when(below[d] > 0)
                    def _():
                        s_wait(s, c)

                    def some(i, carry):
                        at = pl.ds(pl.multiple_of(c * tall + i * step, step), step)
                        accs = sums(s, at, tuple(gin[s, j, at, :].astype(F32) for j in range(half)))
                        for j in range(half):
                            gin[s, j, at, :] = accs[j].astype(BF16)
                        return carry

                    lax.fori_loop(0, tall // step, some, 0)
                    s_copy(d, s, c).start()

    for k in range(1, Q):
        t_copy(k, line(k)).wait_recv()

    feats(0)
    grads(0)
    lasts = lax.fori_loop(0, slots, own_back, (jnp.int32(0),) * half, unroll=unroll)
    for j in range(half):
        base[j] = buf[lasts[j]]
    feats(1)
    grads(1)
    lasts = lax.fori_loop(0, slots, own_fwd, (jnp.int32(0),) * blocks, unroll=unroll)
    lasts = slot_group(0, lasts)
    feats(2)
    back_send(z)
    grads(2)
    for g in range(1, Q):
        lasts = slot_group(g, lasts)

    for r in range(blocks):
        part[r * blk:(r + 1) * blk, :] = buf[lasts[r]].astype(BF16)
    for j in range(half):
        psend[j] = buf[jnp.where(col == 0, lasts[half + j], lasts[j])]
    p_copy = remote(psend, precv, misc.at[6], misc.at[7], me, other)
    p_copy.start()
    term = lax.dot_general(part[...], cot[...], (((0,), (0,)), ((), ())),
                           preferred_element_type=F32) * jnp.float32(scale)
    wchunk[...] = term.astype(BF16).reshape(wchunk.shape)

    first, doms = owners
    held = 2 * doms
    mine = flat - 2 * first
    is_owner = (me >= first) & (me < first + doms)

    def r_copy(o):
        return remote(wchunk.at[o], wpart.at[flat], r_send.at[o], r_recv.at[flat],
                      first + lax.div(o, 2), lax.rem(o, 2))

    def r_in(f):
        return remote(wchunk.at[0], wpart.at[f], r_send.at[0], r_recv.at[f], me, other)

    def others(limit, start, skip, body):
        def step(k, carry):
            at = lax.rem(start + k, limit)

            @pl.when(at != skip)
            def _():
                body(at)
            return carry

        lax.fori_loop(0, limit, step, 0)

    others(held, lax.rem(flat, held), mine, lambda o: r_copy(o).start())

    p_copy.wait()
    for j in range(half):
        whose = buf[jnp.where(col == 0, lasts[j], lasts[half + j])]
        hid[pl.ds(j * blk, blk), :] = (whose + precv[j]).astype(BF16)
    out[...] = jnp.dot(hid[...], weight[...], preferred_element_type=F32).astype(BF16)
    out_copy = pltpu.make_async_copy(out, out_hbm, misc.at[8])
    out_copy.start()

    def g_copy(f):
        return remote(wall.at[mine], wall.at[mine], g_send.at[f], g_recv.at[mine], lax.div(f, 2), lax.rem(f, 2))

    def g_in(o):
        return remote(wall.at[o], wall.at[o], g_send.at[0], g_recv.at[o], me, other)

    @pl.when(is_owner)
    def _():
        wpart[flat] = wchunk[mine]
        others(2 * n, flat, flat, lambda f: r_in(f).wait_recv())
        total = lax.fori_loop(0, 2 * n, lambda f, acc: acc + wpart[f].astype(F32),
                              jnp.zeros(wpart.shape[1:], F32), unroll=4)
        wall[mine] = total.astype(BF16)
        others(2 * n, flat, flat, lambda f: g_copy(f).start())

    peers(lambda peer: pb_copy(z, peer, peer).wait_recv())
    for c in range(CH):
        for d in range(2):
            @pl.when(below[d] > 0)
            def _():
                s_wait(z if d == 0 else Q, c)

    step = 16

    def final(i, carry):
        at = pl.ds(pl.multiple_of(i * step, step), step)
        starts = tuple(base[j, at, :] + gin[z, j, at, :].astype(F32) + gin[Q, j, at, :].astype(F32)
                       for j in range(half))
        accs = sums(z, at, starts)
        for j in range(half):
            fgrad[j, at, :] = accs[j].astype(BF16)
        return carry

    lax.fori_loop(0, blk // step, final, 0)
    fgrad_copy = pltpu.make_async_copy(fgrad, fgrad_hbm, misc.at[9])
    fgrad_copy.start()

    for k in range(1, Q):
        t_copy(k, z).wait_send()
    for s in range(Q):
        def sent(peer, s=s):
            pf_copy(s, peer, w, whole).wait_send()
            pb_copy(s, peer, w).wait_send()

        peers(sent)
    for c in range(CH):
        for d in range(2):
            for k in range(Q - 1):
                @pl.when((k <= below[d]) & (below[d] < top))
                def _():
                    lf_copy(d, k, c).wait_send()

                @pl.when(below[d] <= k)
                def _():
                    s_copy(d, sum_of(k, d), c).wait_send()
    c_copy.wait_send()
    others(held, 0, mine, lambda o: r_copy(o).wait_send())

    others(held, 0, mine, lambda o: g_in(o).wait_recv())
    wgrad[...] = wall[...].astype(F32).reshape(wgrad.shape)
    wgrad_copy = pltpu.make_async_copy(wgrad, wgrad_hbm, misc.at[10])
    wgrad_copy.start()

    @pl.when(is_owner)
    def _():
        others(2 * n, 0, flat, lambda f: g_copy(f).wait_send())

    out_copy.wait()
    fgrad_copy.wait()
    wgrad_copy.wait()


def place(*refs):
    count = (len(refs) - 1) // 3
    sources, targets, held, sem = refs[:count], refs[count:2 * count], refs[2 * count:-1], refs[-1]
    reads = [pltpu.make_async_copy(a, h, sem.at[i]) for i, (a, h) in enumerate(zip(sources, held))]
    writes = [pltpu.make_async_copy(h, b, sem.at[count + i]) for i, (h, b) in enumerate(zip(held, targets))]
    for read in reads:
        read.start()
    for read, write in zip(reads, writes):
        read.wait()
        write.start()
    for write in writes:
        write.wait()


def finish(*arrays):
    hbm = pl.BlockSpec(memory_space=pl.ANY)
    return pl.pallas_call(
        place,
        out_shape=tuple(jax.ShapeDtypeStruct(a.shape, a.dtype) for a in arrays),
        in_specs=[hbm] * len(arrays),
        out_specs=(hbm,) * len(arrays),
        scratch_shapes=[pltpu.VMEM(a.shape, a.dtype) for a in arrays]
        + [pltpu.SemaphoreType.DMA((2 * len(arrays),))],
    )(*arrays)


def local(features, weight, cotangent, tile_values, tile_rows, tile_cols, tile_count, send_blocks):
    slots, blk, _ = tile_values.shape
    rows, width = features.shape
    width_out = cotangent.shape[1]
    half = rows // blk
    n = send_blocks.shape[1]
    plane = n // Q
    nodes = rows * lax.axis_size("col") * lax.axis_size("dom")
    scale = 1.0 / nodes**0.5
    bf = jnp.bfloat16
    doms = min(n // 2, width // 16)
    owners = (n // 4, doms)
    chunk = width // (2 * doms)
    hbm = pl.BlockSpec(memory_space=pl.ANY)
    smem = pl.BlockSpec(memory_space=pltpu.SMEM)
    sems = pltpu.SemaphoreType.DMA
    out, fgrad, wgrad = pl.pallas_call(
        functools.partial(kernel, scale, owners),
        out_shape=(
            jax.ShapeDtypeStruct((rows, width_out), bf),
            jax.ShapeDtypeStruct((half, blk, width), bf),
            jax.ShapeDtypeStruct((width, width_out), F32),
        ),
        in_specs=[smem] * 4 + [hbm] * 4,
        out_specs=(hbm, hbm, hbm),
        scratch_shapes=[
            pltpu.VMEM((half, blk, width), bf),
            pltpu.VMEM((width, width_out), bf),
            pltpu.VMEM((2 * rows, width_out), bf),
            pltpu.VMEM((slots, blk, blk), bf),
            pltpu.VMEM((Q, plane, blk, width), bf),
            pltpu.VMEM((Q, plane, blk, width), bf),
            pltpu.VMEM((Q, plane, blk, width), bf),
            pltpu.VMEM((Q, plane, blk, width), bf),
            pltpu.VMEM((Q + 1, half, blk, width), bf),
            pltpu.VMEM((slots + 1 + n, blk, width), F32),
            pltpu.VMEM((half, blk, width), F32),
            pltpu.VMEM((2 * half, blk, width), bf),
            pltpu.VMEM((half, blk, width), F32),
            pltpu.VMEM((half, blk, width), F32),
            pltpu.VMEM((rows, width), bf),
            pltpu.VMEM((2 * rows, width), bf),
            pltpu.VMEM((rows, width_out), bf),
            pltpu.VMEM((half, blk, width), bf),
            pltpu.VMEM((width, width_out), F32),
            pltpu.VMEM((2 * doms, chunk, width_out), bf),
            pltpu.VMEM((2 * n, chunk, width_out), bf),
            pltpu.VMEM((2 * doms, chunk, width_out), bf),
            pltpu.SMEM((n,), jnp.int32),
            pltpu.SMEM((Q, n), jnp.int32),
        ] + [pltpu.VMEM((half, blk // CH, width), bf)] * (2 * (Q - 1) * CH) + [
            sems((Q,)), sems((Q,)),
            sems((2, Q - 1, CH)), sems((2, Q - 1, CH)),
            sems((Q, CH)), sems((Q + 1, CH)),
        ] + [sems((Q, plane))] * 4 + [
            sems((2 * doms,)), sems((2 * n,)), sems((2 * n,)), sems((2 * doms,)), sems((11,)),
        ],
        compiler_params=pltpu.CompilerParams(
            collective_id=0, has_side_effects=True, vmem_limit_bytes=67000000),
    )(tile_rows, tile_cols, tile_count, send_blocks.reshape(n),
      features.reshape(half, blk, width), weight, cotangent, tile_values)
    return finish(out, fgrad.reshape(rows, width), wgrad)


def solution(mesh):
    return jax.shard_map(
        local,
        mesh=mesh,
        in_specs=(
            P(("dom", "col"), None),
            P(),
            P(("dom", "col"), None),
            P(("dom", "col"), None, None),
            P(("dom", "col")),
            P(("dom", "col")),
            P(("dom", "col")),
            P(("dom", "col"), None),
        ),
        out_specs=(P(("dom", "col"), None), P(("dom", "col"), None), P()),
        check_vma=False,
    )
```

```python
import functools

import jax
import jax.numpy as jnp
from jax import lax
from jax.experimental import pallas as pl
from jax.experimental.pallas import tpu as pltpu
from jax.sharding import PartitionSpec as P

MESH = pl.DeviceIdType.MESH
F32 = jnp.float32
BF16 = jnp.bfloat16
Q = 4
CH = 4


def kernel(scale, owners, rows_s, cols_s, count_s, send_s, feat_hbm, weight_hbm, cot_hbm, tiles_hbm,
           out_hbm, fgrad_hbm, wgrad_hbm,
           feat, weight, cot, tiles, sendf, recvf, sendb, recvb, gin, buf, base, gh, psend, precv, hid,
           part, out, fgrad, wgrad, wchunk, wpart, wall, tos, table, *rest):
    lines = rest[:2 * (Q - 1) * CH]
    (t_send, t_recv, lf_send, s_send, l_recv, pf_send, pf_recv, pb_send, pb_recv,
     r_send, r_recv, g_send, g_recv, misc) = rest[2 * (Q - 1) * CH:]
    slots = tiles.shape[0]
    half, blk, width = feat.shape
    plane = recvf.shape[1]
    n = Q * plane
    blocks = 2 * half
    top = Q - 1
    tall = blk // CH
    me = lax.axis_index("dom")
    col = lax.axis_index("col")
    other = 1 - col
    count = count_s[0]
    z, w = lax.div(me, plane), lax.rem(me, plane)
    below = (z, top - z)
    flat = 2 * me + col

    def remote(src, dst, s_sem, r_sem, dom, core):
        return pltpu.make_async_remote_copy(
            src_ref=src, dst_ref=dst, send_sem=s_sem, recv_sem=r_sem,
            device_id=(dom, core), device_id_type=MESH)

    def line(k):
        return lax.rem(z + k, Q)

    def peers(body):
        def step(k, carry):
            body(lax.rem(w + k, plane))
            return carry

        lax.fori_loop(1, plane, step, 0)

    feat_copy = pltpu.make_async_copy(feat_hbm, feat, misc.at[0])
    feat_copy.start()
    barrier = pltpu.get_barrier_semaphore()

    def greet(dom, core):
        pl.semaphore_signal(barrier, inc=1, device_id=(dom, core), device_id_type=MESH)

    for k in range(1, Q):
        greet(line(k) * plane + w, col)
    peers(lambda peer: greet(z * plane + peer, col))
    greet(me, other)
    rows = half * blk
    cot_half = cot.at[pl.ds(pl.multiple_of(col * rows, rows), rows)]
    cot_copy = pltpu.make_async_copy(cot_hbm, cot_half, misc.at[1])
    cot_copy.start()
    weight_copy = pltpu.make_async_copy(weight_hbm, weight, misc.at[2])
    weight_copy.start()
    tile_copy = pltpu.make_async_copy(tiles_hbm, tiles, misc.at[3])
    tile_copy.start()

    gin[...] = jnp.zeros(gin.shape, gin.dtype)
    buf[0] = jnp.zeros((blk, width), F32)

    def keep(i, carry):
        table[z, i] = send_s[i]
        return carry

    lax.fori_loop(0, n, keep, 0)

    def part_of(c):
        return pl.ds(c * tall, tall)

    def pf_copy(s, peer, slot, at):
        return remote(sendf.at[s, peer, at], recvf.at[s, slot, at], pf_send, pf_recv.at[s],
                      z * plane + peer, col)

    def pb_copy(s, peer, slot):
        return remote(sendb.at[s, peer], recvb.at[s, slot], pb_send, pb_recv.at[s],
                      z * plane + peer, col)

    whole = pl.ds(0, blk)

    def done(ref, sem):
        return remote(ref, ref, sem, sem, me, other)

    def from_peers(buffer, sem, s):
        done(buffer.at[s, pl.ds(0, plane - 1)], sem.at[s]).wait_recv()

    def spread(source, s, at):
        def one(peer):
            sendf[s, peer, at, :] = source[table[s, z * plane + peer]]

        peers(one)
        peers(lambda peer: pf_copy(s, peer, w, at).start())
        recvf[s, w, at, :] = source[table[s, me]]

    def lf_copy(d, k, c):
        nxt = z + 1 if d == 0 else z - 1
        src = feat.at[:, part_of(c)] if k == 0 else lines[(d * top + k - 1) * CH + c]
        return remote(src, lines[(d * top + k) * CH + c], lf_send.at[d], l_recv.at[d, k, c],
                      nxt * plane + w, col)

    def s_copy(d, k, s, c):
        nxt = z + 1 if d == 0 else z - 1
        slot = s if d == 0 else jnp.where(s == nxt, Q, s)
        return remote(gin.at[s, :, part_of(c)], gin.at[slot, :, part_of(c)], s_send.at[d], l_recv.at[d, k + 1, c],
                      nxt * plane + w, col)

    def s_wait(d, k, slot, c):
        done(gin.at[slot, :, part_of(c)], l_recv.at[d, k, c]).wait_recv()

    def t_copy(k, slot):
        return remote(send_s, table.at[slot], t_send, t_recv, line(k) * plane + w, col)

    feat_copy.wait()
    pl.semaphore_wait(barrier, top + plane)

    for k in range(1, Q):
        t_copy(k, z).start()
    for c in range(CH):
        for d in range(2):
            @pl.when(below[d] < top)
            def _():
                lf_copy(d, 0, c).start()

    spread(feat, z, whole)
    cot_copy.wait()
    c_copy = remote(cot_half, cot_half, misc.at[4], misc.at[5], me, other)
    c_copy.start()

    def find(s, carry):
        found = jnp.int32(0)
        for t in range(slots):
            found = jnp.where((cols_s[t] == s + half) & (t < count), t + 1, found)
        tos[s] = found
        return carry

    lax.fori_loop(0, n, find, 0)
    weight_copy.wait()
    cot_other = cot.at[pl.ds(pl.multiple_of(other * rows, rows), rows)]
    remote(cot_other, cot_other, misc.at[4], misc.at[5], me, other).wait_recv()
    gh[...] = lax.dot_general(cot[...], weight[...], (((1,), (1,)), ((), ())),
                              preferred_element_type=F32).astype(BF16).reshape(gh.shape)
    tile_copy.wait()

    def back_term(slot):
        found = tos[slot]
        at = jnp.maximum(found - 1, 0)
        term = lax.dot_general(tiles[at], gh[rows_s[at]], (((0,), (0,)), ((), ())),
                               preferred_element_type=F32)
        return jnp.where(found > 0, term, 0.0).astype(BF16)

    def back_send(s):
        peers(lambda peer: pb_copy(s, peer, w).start())

    low_side = lax.div(z, Q // 2)
    far = top * (1 - low_side)
    near = 2 - low_side
    pair = z + 1 - 2 * lax.rem(z, 2)
    for i, s in enumerate((far, near, pair, z)):
        def fill(k, carry, s=s):
            peer = lax.rem(w + k, plane)
            sendb[s, peer] = back_term(s * plane + peer)
            return carry

        lax.fori_loop(0, plane, fill, 0, unroll=4)
        recvb[s, w] = sendb[s, w]
        if i == 0:
            back_send(s)

    def link(lasts, key, index):
        prev = jnp.int32(0)
        for r, last in enumerate(lasts):
            prev = jnp.where(key == r, last, prev)
        return prev, tuple(jnp.where(key == r, index, last) for r, last in enumerate(lasts))

    def own_back(t, lasts):
        key = jnp.where(t < count, cols_s[t], -1)
        prev, lasts = link(lasts, key, t + 1)
        term = lax.dot_general(tiles[t], gh[rows_s[t]], (((0,), (0,)), ((), ())),
                               preferred_element_type=F32)
        buf[t + 1] = buf[prev] + term
        return lasts

    unroll = 4 if slots % 4 == 0 else 1

    def own_fwd(t, lasts):
        source = cols_s[t]
        key = jnp.where((t < count) & (source < half), rows_s[t], -1)
        prev, lasts = link(lasts, key, t + 1)
        term = jnp.dot(tiles[t], feat[jnp.minimum(source, half - 1)], preferred_element_type=F32)
        buf[t + 1] = buf[prev] + term
        return lasts

    def slot_group(g, lasts):
        if g == 0:
            s = z
        else:
            zm = z + low_side * (top - 2 * z)
            rel = g - 1 + jnp.where(g <= zm, 0, 1)
            s = rel + low_side * (top - 2 * rel)
        from_peers(recvf, pf_recv, s)

        def step(k, lasts):
            slot = lax.rem(w + k, plane)
            found = tos[s * plane + slot]
            at = jnp.maximum(found - 1, 0)
            key = jnp.where(found > 0, rows_s[at], -1)
            index = slots + 1 + g * plane + k
            prev, lasts = link(lasts, key, index)
            term = jnp.dot(tiles[at], recvf[s, slot], preferred_element_type=F32)
            buf[index] = buf[prev] + term
            return lasts

        return lax.fori_loop(0, plane, step, lasts, unroll=4)

    def sums(s, at, starts):
        def add(slot, accs):
            value = recvb[s, slot, at, :].astype(F32)
            home = table[s, z * plane + slot]
            return tuple(acc + jnp.where(home == j, value, 0.0) for j, acc in enumerate(accs))

        return lax.fori_loop(0, plane, add, starts, unroll=4)

    def sum_of(k, d):
        rel = top - (k - below[d])
        return rel if d == 0 else top - rel

    def feat_of(k, d):
        rel = below[d] - 1 - k
        return rel if d == 0 else top - rel

    def feats(k):
        for c in range(CH):
            for d in range(2):
                @pl.when(k < below[d])
                def _():
                    lf_copy(d, k, c).wait_recv()

                    if k + 1 < top:
                        @pl.when(below[d] < top)
                        def _():
                            lf_copy(d, k + 1, c).start()

            for d in range(2):
                @pl.when(k < below[d])
                def _():
                    spread(lines[(d * top + k) * CH + c], feat_of(k, d), part_of(c))

    is_end = (z == 0) | (z == top)

    def grads(k):
        for d in range(2):
            @pl.when(below[d] <= k)
            def _():
                from_peers(recvb, pb_recv, sum_of(k, d))

        step = tall // 2
        for c in range(CH):
            for d in range(2):
                @pl.when(below[d] <= k)
                def _():
                    s = sum_of(k, d)

                    @pl.when(below[d] > 0)
                    def _():
                        s_wait(d, k, s, c)

                    def some(i, carry):
                        at = pl.ds(pl.multiple_of(c * tall + i * step, step), step)
                        accs = sums(s, at, tuple(gin[s, j, at, :].astype(F32) for j in range(half)))
                        for j in range(half):
                            gin[s, j, at, :] = accs[j].astype(BF16)
                        return carry

                    lax.fori_loop(0, tall // step, some, 0)
                    s_copy(d, k, s, c).start()

    done(table.at[pl.ds(0, top)], t_recv).wait_recv()

    feats(0)
    back_send(near)
    grads(0)
    lasts = lax.fori_loop(0, slots, own_back, (jnp.int32(0),) * half, unroll=unroll)
    for j in range(half):
        base[j] = buf[lasts[j]]
    feats(1)
    grads(1)
    lasts = lax.fori_loop(0, slots, own_fwd, (jnp.int32(0),) * blocks, unroll=unroll)
    lasts = slot_group(0, lasts)
    lasts = slot_group(1, lasts)
    feats(2)
    back_send(pair)
    back_send(z)
    lasts = slot_group(2, lasts)

    @pl.when(jnp.logical_not(is_end))
    def _():
        grads(2)

    lasts = slot_group(3, lasts)

    for r in range(blocks):
        part[r * blk:(r + 1) * blk, :] = buf[lasts[r]].astype(BF16)
    for j in range(half):
        psend[j] = buf[jnp.where(col == 0, lasts[half + j], lasts[j])]
    p_copy = remote(psend, precv, misc.at[6], misc.at[7], me, other)
    p_copy.start()
    term = lax.dot_general(part[...], cot[...], (((0,), (0,)), ((), ())),
                           preferred_element_type=F32) * jnp.float32(scale)
    wchunk[...] = term.astype(BF16).reshape(wchunk.shape)

    first, doms = owners
    held = 2 * doms
    mine = flat - 2 * first
    is_owner = (me >= first) & (me < first + doms)

    def r_copy(o):
        return remote(wchunk.at[o], wpart.at[flat], r_send, r_recv,
                      first + lax.div(o, 2), lax.rem(o, 2))

    def others(limit, start, skip, body):
        def step(k, carry):
            at = lax.rem(start + k, limit)

            @pl.when(at != skip)
            def _():
                body(at)
            return carry

        lax.fori_loop(0, limit, step, 0)

    others(held, lax.rem(flat, held), mine, lambda o: r_copy(o).start())

    @pl.when(is_end)
    def _():
        grads(2)

    p_copy.wait()
    for j in range(half):
        whose = buf[jnp.where(col == 0, lasts[j], lasts[half + j])]
        hid[pl.ds(j * blk, blk), :] = (whose + precv[j]).astype(BF16)
    out[...] = jnp.dot(hid[...], weight[...], preferred_element_type=F32).astype(BF16)
    out_copy = pltpu.make_async_copy(out, out_hbm, misc.at[0])
    out_copy.start()

    def g_copy(f):
        return remote(wall.at[mine], wall.at[mine], g_send, g_recv, lax.div(f, 2), lax.rem(f, 2))

    @pl.when(is_owner)
    def _():
        wpart[flat] = wchunk[mine]
        done(wpart.at[pl.ds(0, 2 * n - 1)], r_recv).wait_recv()
        total = lax.fori_loop(0, 2 * n, lambda f, acc: acc + wpart[f].astype(F32),
                              jnp.zeros(wpart.shape[1:], F32), unroll=4)
        wall[mine] = total.astype(BF16)
        others(2 * n, flat, flat, lambda f: g_copy(f).start())

    from_peers(recvb, pb_recv, z)
    for c in range(CH):
        for d in range(2):
            @pl.when(below[d] > 0)
            def _():
                s_wait(d, top, z if d == 0 else Q, c)

    step = 16

    def final(i, carry):
        at = pl.ds(pl.multiple_of(i * step, step), step)
        starts = tuple(base[j, at, :] + gin[z, j, at, :].astype(F32) + gin[Q, j, at, :].astype(F32)
                       for j in range(half))
        accs = sums(z, at, starts)
        for j in range(half):
            fgrad[j, at, :] = accs[j].astype(BF16)
        return carry

    lax.fori_loop(0, blk // step, final, 0)
    fgrad_copy = pltpu.make_async_copy(fgrad, fgrad_hbm, misc.at[1])
    fgrad_copy.start()

    done(table.at[pl.ds(0, top)], t_send).wait_send()
    done(sendf.at[:, pl.ds(0, plane - 1)], pf_send).wait_send()
    done(sendb.at[:, pl.ds(0, plane - 1)], pb_send).wait_send()
    for d in range(2):
        for k in range(top):
            @pl.when(below[d] == k)
            def _():
                done(gin.at[pl.ds(0, k + 1)], lf_send.at[d]).wait_send()
                done(gin.at[pl.ds(0, top - k)], s_send.at[d]).wait_send()
    c_copy.wait_send()

    @pl.when(is_owner)
    def _():
        done(wchunk.at[pl.ds(0, held - 1)], r_send).wait_send()
        done(wchunk.at[pl.ds(0, held - 1)], g_recv).wait_recv()

    @pl.when(jnp.logical_not(is_owner))
    def _():
        done(wchunk, r_send).wait_send()
        done(wchunk, g_recv).wait_recv()

    wgrad[...] = wall[...].astype(F32).reshape(wgrad.shape)
    wgrad_copy = pltpu.make_async_copy(wgrad, wgrad_hbm, misc.at[2])
    wgrad_copy.start()

    @pl.when(is_owner)
    def _():
        done(wpart.at[pl.ds(0, 2 * n - 1)], g_send).wait_send()

    out_copy.wait()
    fgrad_copy.wait()
    wgrad_copy.wait()


def place(*refs):
    count = (len(refs) - 1) // 3
    sources, targets, held, sem = refs[:count], refs[count:2 * count], refs[2 * count:-1], refs[-1]
    reads = [pltpu.make_async_copy(a, h, sem.at[i]) for i, (a, h) in enumerate(zip(sources, held))]
    writes = [pltpu.make_async_copy(h, b, sem.at[count + i]) for i, (h, b) in enumerate(zip(held, targets))]
    for read in reads:
        read.start()
    for read, write in zip(reads, writes):
        read.wait()
        write.start()
    for write in writes:
        write.wait()


def finish(*arrays):
    hbm = pl.BlockSpec(memory_space=pl.ANY)
    return pl.pallas_call(
        place,
        out_shape=tuple(jax.ShapeDtypeStruct(a.shape, a.dtype) for a in arrays),
        in_specs=[hbm] * len(arrays),
        out_specs=(hbm,) * len(arrays),
        scratch_shapes=[pltpu.VMEM(a.shape, a.dtype) for a in arrays]
        + [pltpu.SemaphoreType.DMA((2 * len(arrays),))],
    )(*arrays)


def local(features, weight, cotangent, tile_values, tile_rows, tile_cols, tile_count, send_blocks):
    slots, blk, _ = tile_values.shape
    rows, width = features.shape
    width_out = cotangent.shape[1]
    half = rows // blk
    n = send_blocks.shape[1]
    plane = n // Q
    nodes = rows * lax.axis_size("col") * lax.axis_size("dom")
    scale = 1.0 / nodes**0.5
    bf = jnp.bfloat16
    doms = min(n // 2, width // 16)
    owners = (n // 4, doms)
    chunk = width // (2 * doms)
    hbm = pl.BlockSpec(memory_space=pl.ANY)
    smem = pl.BlockSpec(memory_space=pltpu.SMEM)
    sems = pltpu.SemaphoreType.DMA
    out, fgrad, wgrad = pl.pallas_call(
        functools.partial(kernel, scale, owners),
        out_shape=(
            jax.ShapeDtypeStruct((rows, width_out), bf),
            jax.ShapeDtypeStruct((half, blk, width), bf),
            jax.ShapeDtypeStruct((width, width_out), F32),
        ),
        in_specs=[smem] * 4 + [hbm] * 4,
        out_specs=(hbm, hbm, hbm),
        scratch_shapes=[
            pltpu.VMEM((half, blk, width), bf),
            pltpu.VMEM((width, width_out), bf),
            pltpu.VMEM((2 * rows, width_out), bf),
            pltpu.VMEM((slots, blk, blk), bf),
            pltpu.VMEM((Q, plane, blk, width), bf),
            pltpu.VMEM((Q, plane, blk, width), bf),
            pltpu.VMEM((Q, plane, blk, width), bf),
            pltpu.VMEM((Q, plane, blk, width), bf),
            pltpu.VMEM((Q + 1, half, blk, width), bf),
            pltpu.VMEM((slots + 1 + n, blk, width), F32),
            pltpu.VMEM((half, blk, width), F32),
            pltpu.VMEM((2 * half, blk, width), bf),
            pltpu.VMEM((half, blk, width), F32),
            pltpu.VMEM((half, blk, width), F32),
            pltpu.VMEM((rows, width), bf),
            pltpu.VMEM((2 * rows, width), bf),
            pltpu.VMEM((rows, width_out), bf),
            pltpu.VMEM((half, blk, width), bf),
            pltpu.VMEM((width, width_out), F32),
            pltpu.VMEM((2 * doms, chunk, width_out), bf),
            pltpu.VMEM((2 * n, chunk, width_out), bf),
            pltpu.VMEM((2 * doms, chunk, width_out), bf),
            pltpu.SMEM((n,), jnp.int32),
            pltpu.SMEM((Q, n), jnp.int32),
        ] + [pltpu.VMEM((half, blk // CH, width), bf)] * (2 * (Q - 1) * CH) + [
            sems(()), sems(()), sems((2,)), sems((2,)), sems((2, Q, CH)),
            sems(()), sems((Q,)), sems(()), sems((Q,)),
            sems(()), sems(()), sems(()), sems(()), sems((8,)),
        ],
        compiler_params=pltpu.CompilerParams(
            collective_id=0, has_side_effects=True, vmem_limit_bytes=67000000),
    )(tile_rows, tile_cols, tile_count, send_blocks.reshape(n),
      features.reshape(half, blk, width), weight, cotangent, tile_values)
    return finish(out, fgrad.reshape(rows, width), wgrad)


def solution(mesh):
    return jax.shard_map(
        local,
        mesh=mesh,
        in_specs=(
            P(("dom", "col"), None),
            P(),
            P(("dom", "col"), None),
            P(("dom", "col"), None, None),
            P(("dom", "col")),
            P(("dom", "col")),
            P(("dom", "col")),
            P(("dom", "col"), None),
        ),
        out_specs=(P(("dom", "col"), None), P(("dom", "col"), None), P()),
        check_vma=False,
    )
```

```python
import functools

import jax
import jax.numpy as jnp
from jax import lax
from jax.experimental import pallas as pl
from jax.experimental.pallas import tpu as pltpu
from jax.sharding import PartitionSpec as P

MESH = pl.DeviceIdType.MESH
F32 = jnp.float32
BF16 = jnp.bfloat16
Q = 4
CH = 4


def kernel(scale, owners, rows_hbm, cols_hbm, count_s, send_hbm, feat_hbm, weight_hbm, cot_hbm, tiles_hbm,
           out, fgrad, wgrad,
           feat, weight, cot, tiles, sendf, recvf, sendb, recvb, gin, buf, base, gh, psend, precv, hid,
           part, wterm, whalf, wpeer, wchunk, wpart, wall, tos, table,
           rows_s, cols_s, send_s, *rest):
    lines = rest[:2 * (Q - 1) * CH]
    (t_send, t_recv, lf_send, s_send, l_recv, pf_send, pf_recv, pb_send, pb_recv,
     r_send, r_recv, g_send, g_recv, misc) = rest[2 * (Q - 1) * CH:]
    slots = tiles.shape[0]
    half, blk, width = feat.shape
    plane = recvf.shape[1]
    n = Q * plane
    blocks = 2 * half
    top = Q - 1
    tall = blk // CH
    me = lax.axis_index("dom")
    col = lax.axis_index("col")
    other = 1 - col
    count = count_s[0]
    z, w = lax.div(me, plane), lax.rem(me, plane)
    below = (z, top - z)

    def remote(src, dst, s_sem, r_sem, dom, core):
        return pltpu.make_async_remote_copy(
            src_ref=src, dst_ref=dst, send_sem=s_sem, recv_sem=r_sem,
            device_id=(dom, core), device_id_type=MESH)

    def line(k):
        return lax.rem(z + k, Q)

    def peers(body):
        def step(k, carry):
            body(lax.rem(w + k, plane))
            return carry

        lax.fori_loop(1, plane, step, 0)

    feat_copy = pltpu.make_async_copy(feat_hbm, feat, misc.at[0])
    feat_copy.start()
    smalls = [pltpu.make_async_copy(a, b, misc.at[12 + i]) for i, (a, b) in enumerate(
        ((send_hbm, send_s), (rows_hbm, rows_s), (cols_hbm, cols_s)))]
    for small in smalls:
        small.start()
    barrier = pltpu.get_barrier_semaphore()

    def greet(dom, core):
        pl.semaphore_signal(barrier, inc=1, device_id=(dom, core), device_id_type=MESH)

    for k in range(1, Q):
        greet(line(k) * plane + w, col)
    peers(lambda peer: greet(z * plane + peer, col))
    greet(me, other)
    rows = half * blk
    cot_half = cot.at[pl.ds(pl.multiple_of(col * rows, rows), rows)]
    cot_copy = pltpu.make_async_copy(cot_hbm, cot_half, misc.at[1])
    cot_copy.start()
    weight_copy = pltpu.make_async_copy(weight_hbm, weight, misc.at[2])
    weight_copy.start()
    tile_copy = pltpu.make_async_copy(tiles_hbm, tiles, misc.at[3])
    tile_copy.start()

    gin[...] = jnp.zeros(gin.shape, gin.dtype)
    buf[0] = jnp.zeros((blk, width), F32)

    for small in smalls:
        small.wait()

    def keep(i, carry):
        table[z, i] = send_s[i]
        return carry

    lax.fori_loop(0, n, keep, 0)

    def part_of(c):
        return pl.ds(c * tall, tall)

    def pf_copy(s, peer, slot, at):
        return remote(sendf.at[s, peer, at], recvf.at[s, slot, at], pf_send, pf_recv.at[s],
                      z * plane + peer, col)

    def pb_copy(s, peer, slot):
        return remote(sendb.at[s, peer], recvb.at[s, slot], pb_send, pb_recv.at[s],
                      z * plane + peer, col)

    whole = pl.ds(0, blk)

    def done(ref, sem):
        return remote(ref, ref, sem, sem, me, other)

    def from_peers(buffer, sem, s):
        done(buffer.at[s, pl.ds(0, plane - 1)], sem.at[s]).wait_recv()

    def spread(source, s, at):
        def one(peer):
            sendf[s, peer, at, :] = source[table[s, z * plane + peer]]

        peers(one)
        peers(lambda peer: pf_copy(s, peer, w, at).start())
        recvf[s, w, at, :] = source[table[s, me]]

    def lf_copy(d, k, c):
        nxt = z + 1 if d == 0 else z - 1
        src = feat.at[:, part_of(c)] if k == 0 else lines[(d * top + k - 1) * CH + c]
        return remote(src, lines[(d * top + k) * CH + c], lf_send.at[d], l_recv.at[d, k, c],
                      nxt * plane + w, col)

    def s_copy(d, k, s, c):
        nxt = z + 1 if d == 0 else z - 1
        slot = s if d == 0 else jnp.where(s == nxt, Q, s)
        return remote(gin.at[s, :, part_of(c)], gin.at[slot, :, part_of(c)], s_send.at[d], l_recv.at[d, k + 1, c],
                      nxt * plane + w, col)

    def s_wait(d, k, slot, c):
        done(gin.at[slot, :, part_of(c)], l_recv.at[d, k, c]).wait_recv()

    def t_copy(k, slot):
        return remote(send_s, table.at[slot], t_send, t_recv, line(k) * plane + w, col)

    feat_copy.wait()
    pl.semaphore_wait(barrier, top + plane)

    for k in range(1, Q):
        t_copy(k, z).start()
    for c in range(CH):
        for d in range(2):
            @pl.when(below[d] < top)
            def _():
                lf_copy(d, 0, c).start()

    spread(feat, z, whole)
    cot_copy.wait()
    c_copy = remote(cot_half, cot_half, misc.at[4], misc.at[5], me, other)
    c_copy.start()

    def find(s, carry):
        found = jnp.int32(0)
        for t in range(slots):
            found = jnp.where((cols_s[t] == s + half) & (t < count), t + 1, found)
        tos[s] = found
        return carry

    lax.fori_loop(0, n, find, 0)
    weight_copy.wait()
    cot_other = cot.at[pl.ds(pl.multiple_of(other * rows, rows), rows)]
    remote(cot_other, cot_other, misc.at[4], misc.at[5], me, other).wait_recv()
    gh[...] = lax.dot_general(cot[...], weight[...], (((1,), (1,)), ((), ())),
                              preferred_element_type=F32).astype(BF16).reshape(gh.shape)
    tile_copy.wait()

    def back_term(slot):
        found = tos[slot]
        at = jnp.maximum(found - 1, 0)
        term = lax.dot_general(tiles[at], gh[rows_s[at]], (((0,), (0,)), ((), ())),
                               preferred_element_type=F32)
        return jnp.where(found > 0, term, 0.0).astype(BF16)

    def back_send(s):
        peers(lambda peer: pb_copy(s, peer, w).start())

    low_side = lax.div(z, Q // 2)
    far = top * (1 - low_side)
    near = 2 - low_side
    pair = z + 1 - 2 * lax.rem(z, 2)
    for i, s in enumerate((far, near, pair, z)):
        def fill(k, carry, s=s):
            peer = lax.rem(w + k, plane)
            sendb[s, peer] = back_term(s * plane + peer)
            return carry

        lax.fori_loop(0, plane, fill, 0, unroll=4)
        recvb[s, w] = sendb[s, w]
        if i == 0:
            back_send(s)

    def link(lasts, key, index):
        prev = jnp.int32(0)
        for r, last in enumerate(lasts):
            prev = jnp.where(key == r, last, prev)
        return prev, tuple(jnp.where(key == r, index, last) for r, last in enumerate(lasts))

    def own_back(t, lasts):
        key = jnp.where(t < count, cols_s[t], -1)
        prev, lasts = link(lasts, key, t + 1)
        term = lax.dot_general(tiles[t], gh[rows_s[t]], (((0,), (0,)), ((), ())),
                               preferred_element_type=F32)
        buf[t + 1] = buf[prev] + term
        return lasts

    unroll = 4 if slots % 4 == 0 else 1

    def own_fwd(t, lasts):
        source = cols_s[t]
        key = jnp.where((t < count) & (source < half), rows_s[t], -1)
        prev, lasts = link(lasts, key, t + 1)
        term = jnp.dot(tiles[t], feat[jnp.minimum(source, half - 1)], preferred_element_type=F32)
        buf[t + 1] = buf[prev] + term
        return lasts

    def slot_group(g, lasts):
        if g == 0:
            s = z
        else:
            zm = z + low_side * (top - 2 * z)
            rel = g - 1 + jnp.where(g <= zm, 0, 1)
            s = rel + low_side * (top - 2 * rel)
        from_peers(recvf, pf_recv, s)

        def step(k, lasts):
            slot = lax.rem(w + k, plane)
            found = tos[s * plane + slot]
            at = jnp.maximum(found - 1, 0)
            key = jnp.where(found > 0, rows_s[at], -1)
            index = slots + 1 + g * plane + k
            prev, lasts = link(lasts, key, index)
            term = jnp.dot(tiles[at], recvf[s, slot], preferred_element_type=F32)
            buf[index] = buf[prev] + term
            return lasts

        return lax.fori_loop(0, plane, step, lasts, unroll=4)

    def sums(s, at, starts):
        def add(slot, accs):
            value = recvb[s, slot, at, :].astype(F32)
            home = table[s, z * plane + slot]
            return tuple(acc + jnp.where(home == j, value, 0.0) for j, acc in enumerate(accs))

        return lax.fori_loop(0, plane, add, starts, unroll=4)

    def sum_of(k, d):
        rel = top - (k - below[d])
        return rel if d == 0 else top - rel

    def feat_of(k, d):
        rel = below[d] - 1 - k
        return rel if d == 0 else top - rel

    def feats(k):
        for c in range(CH):
            for d in range(2):
                @pl.when(k < below[d])
                def _():
                    lf_copy(d, k, c).wait_recv()

                    if k + 1 < top:
                        @pl.when(below[d] < top)
                        def _():
                            lf_copy(d, k + 1, c).start()

            for d in range(2):
                @pl.when(k < below[d])
                def _():
                    spread(lines[(d * top + k) * CH + c], feat_of(k, d), part_of(c))

    def grads(k):
        for d in range(2):
            @pl.when(below[d] <= k)
            def _():
                from_peers(recvb, pb_recv, sum_of(k, d))

        step = tall // 2
        for c in range(CH):
            for d in range(2):
                @pl.when(below[d] <= k)
                def _():
                    s = sum_of(k, d)

                    @pl.when(below[d] > 0)
                    def _():
                        s_wait(d, k, s, c)

                    def some(i, carry):
                        at = pl.ds(pl.multiple_of(c * tall + i * step, step), step)
                        accs = sums(s, at, tuple(gin[s, j, at, :].astype(F32) for j in range(half)))
                        for j in range(half):
                            gin[s, j, at, :] = accs[j].astype(BF16)
                        return carry

                    lax.fori_loop(0, tall // step, some, 0)
                    s_copy(d, k, s, c).start()

    lasts = lax.fori_loop(0, slots, own_back, (jnp.int32(0),) * half, unroll=unroll)
    for j in range(half):
        base[j] = buf[lasts[j]]
    done(table.at[pl.ds(0, top)], t_recv).wait_recv()

    is_end = (z == 0) | (z == top)
    feats(0)
    back_send(near)
    grads(0)
    feats(1)
    grads(1)

    @pl.when(jnp.logical_not(is_end))
    def _():
        back_send(pair)
        back_send(z)

    lasts = slot_group(0, (jnp.int32(0),) * blocks)
    feats(2)

    @pl.when(is_end)
    def _():
        back_send(pair)

    lasts = lax.fori_loop(0, slots, own_fwd, lasts, unroll=unroll)
    for g in range(1, Q):
        lasts = slot_group(g, lasts)

    for r in range(blocks):
        part[r * blk:(r + 1) * blk, :] = buf[lasts[r]].astype(BF16)
    wterm[...] = lax.dot_general(part[...], cot[...], (((0,), (0,)), ((), ())),
                                 preferred_element_type=F32) * jnp.float32(scale)
    d_copy = remote(whalf, wpeer, misc.at[8], misc.at[9], me, other)

    @pl.when(col == 0)
    def _():
        whalf[...] = wterm[...].astype(BF16)
        d_copy.start()

    first, doms = owners
    mine = me - first
    is_owner = (col == 1) & (me >= first) & (me < first + doms)

    def others(limit, start, skip, body):
        def step(k, carry):
            at = lax.rem(start + k, limit)

            @pl.when(at != skip)
            def _():
                body(at)
            return carry

        lax.fori_loop(0, limit, step, 0)

    @pl.when(col == 1)
    def _():
        d_copy.wait_recv()
        wchunk[...] = (wterm[...] + wpeer[...].astype(F32)).astype(BF16).reshape(wchunk.shape)
        others(doms, lax.rem(me, doms), mine,
               lambda i: remote(wchunk.at[i], wpart.at[me], r_send, r_recv, first + i, 1).start())

    for j in range(half):
        psend[j] = buf[jnp.where(col == 0, lasts[half + j], lasts[j])]
    p_copy = remote(psend, precv, misc.at[6], misc.at[7], me, other)
    p_copy.start()

    @pl.when(is_end)
    def _():
        back_send(z)

    grads(2)

    p_copy.wait()
    for j in range(half):
        whose = buf[jnp.where(col == 0, lasts[j], lasts[half + j])]
        hid[pl.ds(j * blk, blk), :] = (whose + precv[j]).astype(BF16)
    out[...] = jnp.dot(hid[...], weight[...], preferred_element_type=F32).astype(BF16)

    @pl.when(is_owner)
    def _():
        wpart[me] = wchunk[mine]
        done(wpart.at[pl.ds(0, n - 1)], r_recv).wait_recv()
        total = lax.fori_loop(0, n, lambda f, acc: acc + wpart[f].astype(F32),
                              jnp.zeros(wpart.shape[1:], F32), unroll=4)
        wall[mine] = total.astype(BF16)
        others(n, me, me,
               lambda f: remote(wall.at[mine], wall.at[mine], g_send, g_recv, f, 1).start())

    from_peers(recvb, pb_recv, z)
    for c in range(CH):
        for d in range(2):
            @pl.when(below[d] > 0)
            def _():
                s_wait(d, top, z if d == 0 else Q, c)

    step = 16

    def final(i, carry):
        at = pl.ds(pl.multiple_of(i * step, step), step)
        starts = tuple(base[j, at, :] + gin[z, j, at, :].astype(F32) + gin[Q, j, at, :].astype(F32)
                       for j in range(half))
        accs = sums(z, at, starts)
        for j in range(half):
            fgrad[j, at, :] = accs[j].astype(BF16)
        return carry

    lax.fori_loop(0, blk // step, final, 0)

    done(table.at[pl.ds(0, top)], t_send).wait_send()
    done(sendf.at[:, pl.ds(0, plane - 1)], pf_send).wait_send()
    done(sendb.at[:, pl.ds(0, plane - 1)], pb_send).wait_send()
    for d in range(2):
        for k in range(top):
            @pl.when(below[d] == k)
            def _():
                done(gin.at[pl.ds(0, k + 1)], lf_send.at[d]).wait_send()
                done(gin.at[pl.ds(0, top - k)], s_send.at[d]).wait_send()
    c_copy.wait_send()

    h_copy = remote(wall, wall, misc.at[10], misc.at[11], me, other)

    @pl.when(is_owner)
    def _():
        done(wchunk.at[pl.ds(0, doms - 1)], g_recv).wait_recv()

    @pl.when((col == 1) & jnp.logical_not(is_owner))
    def _():
        done(wchunk, g_recv).wait_recv()

    @pl.when(col == 1)
    def _():
        h_copy.start()

    @pl.when(col == 0)
    def _():
        h_copy.wait_recv()
        d_copy.wait_send()

    wgrad[...] = wall[...].astype(F32).reshape(wgrad.shape)

    @pl.when(is_owner)
    def _():
        done(wchunk.at[pl.ds(0, doms - 1)], r_send).wait_send()
        done(wpart.at[pl.ds(0, n - 1)], g_send).wait_send()

    @pl.when((col == 1) & jnp.logical_not(is_owner))
    def _():
        done(wchunk, r_send).wait_send()

    @pl.when(col == 1)
    def _():
        h_copy.wait_send()


def place(*refs):
    count = len(refs) // 2
    sem = refs[-1]
    writes = [pltpu.make_async_copy(a, b, sem.at[i]) for i, (a, b) in enumerate(zip(refs[:count], refs[count:-1]))]
    for write in writes:
        write.start()
    for write in writes:
        write.wait()


def finish(*arrays):
    return pl.pallas_call(
        place,
        out_shape=tuple(jax.ShapeDtypeStruct(a.shape, a.dtype) for a in arrays),
        in_specs=[pl.BlockSpec(memory_space=pltpu.VMEM)] * len(arrays),
        out_specs=(pl.BlockSpec(memory_space=pltpu.HBM),) * len(arrays),
        scratch_shapes=[pltpu.SemaphoreType.DMA((len(arrays),))],
        compiler_params=pltpu.CompilerParams(vmem_limit_bytes=4000000),
    )(*arrays)


def in_hbm(array):
    return pltpu.with_memory_space_constraint(array, pltpu.HBM)


def local(features, weight, cotangent, tile_values, tile_rows, tile_cols, tile_count, send_blocks):
    slots, blk, _ = tile_values.shape
    rows, width = features.shape
    width_out = cotangent.shape[1]
    half = rows // blk
    n = send_blocks.shape[1]
    plane = n // Q
    nodes = rows * lax.axis_size("col") * lax.axis_size("dom")
    scale = 1.0 / nodes**0.5
    bf = jnp.bfloat16
    doms = min(n // 2, width // 16)
    owners = (n // 4, doms)
    chunk = width // doms
    hbm = pl.BlockSpec(memory_space=pltpu.HBM)
    vmem = pl.BlockSpec(memory_space=pltpu.VMEM)
    smem = pl.BlockSpec(memory_space=pltpu.SMEM)
    sems = pltpu.SemaphoreType.DMA
    out, fgrad, wgrad = pl.pallas_call(
        functools.partial(kernel, scale, owners),
        out_shape=(
            jax.ShapeDtypeStruct((rows, width_out), bf),
            jax.ShapeDtypeStruct((half, blk, width), bf),
            jax.ShapeDtypeStruct((width, width_out), F32),
        ),
        in_specs=[hbm, hbm, smem] + [hbm] * 5,
        out_specs=(vmem, vmem, vmem),
        scratch_shapes=[
            pltpu.VMEM((half, blk, width), bf),
            pltpu.VMEM((width, width_out), bf),
            pltpu.VMEM((2 * rows, width_out), bf),
            pltpu.VMEM((slots, blk, blk), bf),
            pltpu.VMEM((Q, plane, blk, width), bf),
            pltpu.VMEM((Q, plane, blk, width), bf),
            pltpu.VMEM((Q, plane, blk, width), bf),
            pltpu.VMEM((Q, plane, blk, width), bf),
            pltpu.VMEM((Q + 1, half, blk, width), bf),
            pltpu.VMEM((slots + 1 + n, blk, width), F32),
            pltpu.VMEM((half, blk, width), F32),
            pltpu.VMEM((2 * half, blk, width), bf),
            pltpu.VMEM((half, blk, width), F32),
            pltpu.VMEM((half, blk, width), F32),
            pltpu.VMEM((rows, width), bf),
            pltpu.VMEM((2 * rows, width), bf),
            pltpu.VMEM((width, width_out), F32),
            pltpu.VMEM((width, width_out), bf),
            pltpu.VMEM((width, width_out), bf),
            pltpu.VMEM((doms, chunk, width_out), bf),
            pltpu.VMEM((n, chunk, width_out), bf),
            pltpu.VMEM((doms, chunk, width_out), bf),
            pltpu.SMEM((n,), jnp.int32),
            pltpu.SMEM((Q, n), jnp.int32),
            pltpu.SMEM((slots,), jnp.int32),
            pltpu.SMEM((slots,), jnp.int32),
            pltpu.SMEM((n,), jnp.int32),
        ] + [pltpu.VMEM((half, blk // CH, width), bf)] * (2 * (Q - 1) * CH) + [
            sems(()), sems(()), sems((2,)), sems((2,)), sems((2, Q, CH)),
            sems(()), sems((Q,)), sems(()), sems((Q,)),
            sems(()), sems(()), sems(()), sems(()), sems((15,)),
        ],
        compiler_params=pltpu.CompilerParams(
            collective_id=0, has_side_effects=True, vmem_limit_bytes=min(67000000, 20000000 + 12 * n * blk * width)),
    )(in_hbm(tile_rows), in_hbm(tile_cols), tile_count, in_hbm(send_blocks.reshape(n)),
      in_hbm(features.reshape(half, blk, width)), in_hbm(weight), in_hbm(cotangent), in_hbm(tile_values))
    return finish(out, fgrad.reshape(rows, width), wgrad)


def solution(mesh):
    return jax.shard_map(
        local,
        mesh=mesh,
        in_specs=(
            P(("dom", "col"), None),
            P(),
            P(("dom", "col"), None),
            P(("dom", "col"), None, None),
            P(("dom", "col")),
            P(("dom", "col")),
            P(("dom", "col")),
            P(("dom", "col"), None),
        ),
        out_specs=(P(("dom", "col"), None), P(("dom", "col"), None), P()),
        check_vma=False,
    )
```

```python
import functools

import jax
import jax.numpy as jnp
from jax import lax
from jax.experimental import pallas as pl
from jax.experimental.pallas import tpu as pltpu
from jax.sharding import PartitionSpec as P

MESH = pl.DeviceIdType.MESH
F32 = jnp.float32
BF16 = jnp.bfloat16
Q = 4
CH = 4


def kernel(scale, owners, rows_hbm, cols_hbm, count_s, send_hbm, feat_hbm, weight_hbm, cot_hbm, tiles_hbm,
           out, fgrad, wgrad,
           feat, weight, cot, tiles, sendf, recvf, sendb, recvb, gin, buf, base, gh, psend, precv,
           sendx, wchunk, wpart, wall, tos, table,
           rows_s, cols_s, send_s, *rest):
    hops = Q - 2
    lines = rest[:2 * hops * CH]
    (t_send, t_recv, lf_send, s_send, l_recv, pf_send, pf_recv, pb_send, pb_recv,
     x_send, r_send, r_recv, g_send, g_recv, misc) = rest[2 * hops * CH:]
    slots = tiles.shape[0]
    half, blk, width = feat.shape
    plane = recvf.shape[1]
    n = Q * plane
    blocks = 2 * half
    top = Q - 1
    tall = blk // CH
    me = lax.axis_index("dom")
    col = lax.axis_index("col")
    other = 1 - col
    count = count_s[0]
    z, w = lax.div(me, plane), lax.rem(me, plane)
    below = (z, top - z)
    is_end = (z == 0) | (z == top)

    def remote(src, dst, s_sem, r_sem, dom, core):
        return pltpu.make_async_remote_copy(
            src_ref=src, dst_ref=dst, send_sem=s_sem, recv_sem=r_sem,
            device_id=(dom, core), device_id_type=MESH)

    def line(k):
        return lax.rem(z + k, Q)

    def peers(body):
        def step(k, carry):
            body(lax.rem(w + k, plane))
            return carry

        lax.fori_loop(1, plane, step, 0)

    feat_copy = pltpu.make_async_copy(feat_hbm, feat, misc.at[0])
    feat_copy.start()
    smalls = [pltpu.make_async_copy(a, b, misc.at[12 + i]) for i, (a, b) in enumerate(
        ((send_hbm, send_s), (rows_hbm, rows_s), (cols_hbm, cols_s)))]
    for small in smalls:
        small.start()
    barrier = pltpu.get_barrier_semaphore()

    def greet(dom, core):
        pl.semaphore_signal(barrier, inc=1, device_id=(dom, core), device_id_type=MESH)

    for k in range(1, Q):
        greet(line(k) * plane + w, col)
    peers(lambda peer: greet(z * plane + peer, col))
    greet(me, other)
    rows = half * blk
    cot_half = cot.at[pl.ds(pl.multiple_of(col * rows, rows), rows)]
    cot_copy = pltpu.make_async_copy(cot_hbm, cot_half, misc.at[1])
    cot_copy.start()
    weight_copy = pltpu.make_async_copy(weight_hbm, weight, misc.at[2])
    weight_copy.start()
    tile_copy = pltpu.make_async_copy(tiles_hbm, tiles, misc.at[3])
    tile_copy.start()

    gin[...] = jnp.zeros(gin.shape, gin.dtype)
    buf[0] = jnp.zeros((blk, width), F32)

    for small in smalls:
        small.wait()

    def keep(i, carry):
        table[z, i] = send_s[i]
        return carry

    lax.fori_loop(0, n, keep, 0)

    def part_of(c):
        return pl.ds(c * tall, tall)

    def pf_copy(s, peer, slot, at):
        return remote(sendf.at[s, peer, at], recvf.at[s, slot, at], pf_send, pf_recv.at[s],
                      z * plane + peer, col)

    def pb_copy(s, peer, slot):
        return remote(sendb.at[s, peer], recvb.at[s, slot], pb_send, pb_recv.at[s],
                      z * plane + peer, col)

    whole = pl.ds(0, blk)

    def done(ref, sem):
        return remote(ref, ref, sem, sem, me, other)

    def from_peers(buffer, sem, s):
        done(buffer.at[s, pl.ds(0, plane - 1)], sem.at[s]).wait_recv()

    def spread(source, s, at):
        def one(peer):
            sendf[s, peer, at, :] = source[table[s, z * plane + peer]]

        peers(one)
        peers(lambda peer: pf_copy(s, peer, w, at).start())
        recvf[s, w, at, :] = source[table[s, me]]

    def lf_copy(d, k, c):
        nxt = z + 1 if d == 0 else z - 1
        src = feat.at[:, part_of(c)] if k == 0 else lines[(d * hops + k - 1) * CH + c]
        return remote(src, lines[(d * hops + k) * CH + c], lf_send.at[d], l_recv.at[d, k, c],
                      nxt * plane + w, col)

    def s_copy(d, k, s, c):
        nxt = z + 1 if d == 0 else z - 1
        slot = s if d == 0 else jnp.where(s == nxt, Q, s)
        return remote(gin.at[s, :, part_of(c)], gin.at[slot, :, part_of(c)], s_send.at[d], l_recv.at[d, k + 1, c],
                      nxt * plane + w, col)

    def s_wait(d, k, slot, c):
        done(gin.at[slot, :, part_of(c)], l_recv.at[d, k, c]).wait_recv()

    def t_copy(k, slot):
        return remote(send_s, table.at[slot], t_send, t_recv, line(k) * plane + w, col)

    feat_copy.wait()
    pl.semaphore_wait(barrier, top + plane)

    for k in range(1, Q):
        t_copy(k, z).start()
    for c in range(CH):
        for d in range(2):
            @pl.when(below[d] < top)
            def _():
                lf_copy(d, 0, c).start()

    spread(feat, z, whole)
    cot_copy.wait()
    c_copy = remote(cot_half, cot_half, misc.at[4], misc.at[5], me, other)
    c_copy.start()

    def find(s, carry):
        found = jnp.int32(0)
        for t in range(slots):
            found = jnp.where((cols_s[t] == s + half) & (t < count), t + 1, found)
        tos[s] = found
        return carry

    lax.fori_loop(0, n, find, 0)
    weight_copy.wait()
    cot_other = cot.at[pl.ds(pl.multiple_of(other * rows, rows), rows)]
    remote(cot_other, cot_other, misc.at[4], misc.at[5], me, other).wait_recv()
    gh[...] = lax.dot_general(cot[...], weight[...], (((1,), (1,)), ((), ())),
                              preferred_element_type=F32).astype(BF16).reshape(gh.shape)
    tile_copy.wait()

    def back_term(slot):
        found = tos[slot]
        at = jnp.maximum(found - 1, 0)
        term = lax.dot_general(tiles[at], gh[rows_s[at]], (((0,), (0,)), ((), ())),
                               preferred_element_type=F32)
        return jnp.where(found > 0, term, 0.0).astype(BF16)

    def back_send(s):
        peers(lambda peer: pb_copy(s, peer, w).start())

    low_side = lax.div(z, Q // 2)
    far = top * (1 - low_side)
    near = 2 - low_side
    pair = z + 1 - 2 * lax.rem(z, 2)
    for i, s in enumerate((far, near, pair, z)):
        def fill(k, carry, s=s):
            peer = lax.rem(w + k, plane)
            sendb[s, peer] = back_term(s * plane + peer)
            return carry

        lax.fori_loop(0, plane, fill, 0, unroll=4)
        recvb[s, w] = sendb[s, w]
        if i == 0:
            back_send(s)

    def link(lasts, key, index):
        prev = jnp.int32(0)
        for r, last in enumerate(lasts):
            prev = jnp.where(key == r, last, prev)
        return prev, tuple(jnp.where(key == r, index, last) for r, last in enumerate(lasts))

    def own_back(t, lasts):
        key = jnp.where(t < count, cols_s[t], -1)
        prev, lasts = link(lasts, key, t + 1)
        term = lax.dot_general(tiles[t], gh[rows_s[t]], (((0,), (0,)), ((), ())),
                               preferred_element_type=F32)
        buf[t + 1] = buf[prev] + term
        return lasts

    unroll = 4 if slots % 4 == 0 else 1

    def own_fwd(t, lasts):
        source = cols_s[t]
        key = jnp.where((t < count) & (source < half), rows_s[t], -1)
        prev, lasts = link(lasts, key, t + 1)
        term = jnp.dot(tiles[t], feat[jnp.minimum(source, half - 1)], preferred_element_type=F32)
        buf[t + 1] = buf[prev] + term
        return lasts

    def slot_group(g, lasts):
        if g == 0:
            s = z
        else:
            zm = z + low_side * (top - 2 * z)
            rel = g - 1 + jnp.where(g <= zm, 0, 1)
            s = rel + low_side * (top - 2 * rel)
        if g < top:
            from_peers(recvf, pf_recv, s)
        else:
            @pl.when(is_end)
            def _():
                done(recvf.at[s], pf_recv.at[s]).wait_recv()

            @pl.when(jnp.logical_not(is_end))
            def _():
                from_peers(recvf, pf_recv, s)


        def step(k, lasts):
            slot = lax.rem(w + k, plane)
            found = tos[s * plane + slot]
            at = jnp.maximum(found - 1, 0)
            key = jnp.where(found > 0, rows_s[at], -1)
            index = slots + 1 + g * plane + k
            prev, lasts = link(lasts, key, index)
            term = jnp.dot(tiles[at], recvf[s, slot], preferred_element_type=F32)
            buf[index] = buf[prev] + term
            return lasts

        return lax.fori_loop(0, plane, step, lasts, unroll=4)

    def sums(s, at, starts):
        def add(slot, accs):
            value = recvb[s, slot, at, :].astype(F32)
            home = table[s, z * plane + slot]
            return tuple(acc + jnp.where(home == j, value, 0.0) for j, acc in enumerate(accs))

        return lax.fori_loop(0, plane, add, starts, unroll=4)

    def sum_of(k, d):
        rel = top - (k - below[d])
        return rel if d == 0 else top - rel

    def feat_of(k, d):
        rel = below[d] - 1 - k
        return rel if d == 0 else top - rel

    def reach(d, source, s, at):
        nxt = (z + 1 if d == 0 else z - 1) * plane

        def one(k, carry):
            peer = lax.rem(w + k, plane)
            sendx[peer, at, :] = source[table[s, nxt + peer]]
            return carry

        def go(k, carry):
            peer = lax.rem(w + k, plane)
            remote(sendx.at[peer, at], recvf.at[s, w, at], x_send, pf_recv.at[s], nxt + peer, col).start()
            return carry

        lax.fori_loop(0, plane, one, 0)
        lax.fori_loop(0, plane, go, 0)

    def feats(k):
        for c in range(CH):
            for d in range(2):
                @pl.when(k < below[d])
                def _():
                    lf_copy(d, k, c).wait_recv()

                    @pl.when(below[d] < top)
                    def _():
                        if k + 1 < hops:
                            lf_copy(d, k + 1, c).start()
                        else:
                            reach(d, lines[(d * hops + k) * CH + c], feat_of(k, d), part_of(c))

            for d in range(2):
                @pl.when(k < below[d])
                def _():
                    spread(lines[(d * hops + k) * CH + c], feat_of(k, d), part_of(c))

    def grads(k):
        for d in range(2):
            @pl.when(below[d] <= k)
            def _():
                from_peers(recvb, pb_recv, sum_of(k, d))

        step = tall // 2
        for c in range(CH):
            for d in range(2):
                @pl.when(below[d] <= k)
                def _():
                    s = sum_of(k, d)

                    @pl.when(below[d] > 0)
                    def _():
                        s_wait(d, k, s, c)

                    def some(i, carry):
                        at = pl.ds(pl.multiple_of(c * tall + i * step, step), step)
                        accs = sums(s, at, tuple(gin[s, j, at, :].astype(F32) for j in range(half)))
                        for j in range(half):
                            gin[s, j, at, :] = accs[j].astype(BF16)
                        return carry

                    lax.fori_loop(0, tall // step, some, 0)
                    s_copy(d, k, s, c).start()

    lasts = lax.fori_loop(0, slots, own_back, (jnp.int32(0),) * half, unroll=unroll)
    for j in range(half):
        base[j] = buf[lasts[j]]
    done(table.at[pl.ds(0, top)], t_recv).wait_recv()

    feats(0)
    back_send(near)
    grads(0)
    feats(1)
    grads(1)

    back_send(pair)

    @pl.when(jnp.logical_not(is_end))
    def _():
        back_send(z)

    lasts = slot_group(0, (jnp.int32(0),) * blocks)
    lasts = lax.fori_loop(0, slots, own_fwd, lasts, unroll=unroll)
    for g in range(1, Q):
        lasts = slot_group(g, lasts)

    for r in range(blocks):
        gh[r] = buf[lasts[r]].astype(BF16)
    term = lax.dot_general(gh[...].reshape(cot.shape), cot[...], (((0,), (0,)), ((), ())),
                           preferred_element_type=F32) * jnp.float32(scale)
    wchunk[...] = term.astype(BF16).reshape(wchunk.shape)

    first, doms = owners
    mine = me - first
    is_owner = (col == 1) & (me >= first) & (me < first + doms)

    def others(limit, start, skip, body):
        def step(k, carry):
            at = lax.rem(start + k, limit)

            @pl.when(at != skip)
            def _():
                body(at)
            return carry

        lax.fori_loop(0, limit, step, 0)

    flat = 2 * me + col
    keep_own = jnp.where(is_owner, mine, doms)
    others(doms, lax.rem(me, doms), keep_own,
           lambda i: remote(wchunk.at[i], wpart.at[flat], r_send, r_recv, first + i, 1).start())

    for j in range(half):
        psend[j] = buf[jnp.where(col == 0, lasts[half + j], lasts[j])]
    p_copy = remote(psend, precv, misc.at[6], misc.at[7], me, other)
    p_copy.start()

    @pl.when(is_end)
    def _():
        back_send(z)

    grads(2)

    p_copy.wait()
    for j in range(half):
        whose = buf[jnp.where(col == 0, lasts[j], lasts[half + j])]
        hidden = (whose + precv[j]).astype(BF16)
        out[pl.ds(j * blk, blk), :] = jnp.dot(hidden, weight[...], preferred_element_type=F32).astype(BF16)

    @pl.when(is_owner)
    def _():
        wpart[flat] = wchunk[mine]
        done(wpart.at[pl.ds(0, 2 * n - 1)], r_recv).wait_recv()
        total = lax.fori_loop(0, 2 * n, lambda f, acc: acc + wpart[f].astype(F32),
                              jnp.zeros(wpart.shape[1:], F32), unroll=4)
        wall[mine] = total.astype(BF16)
        others(n, me, me,
               lambda f: remote(wall.at[mine], wall.at[mine], g_send, g_recv, f, 1).start())

    from_peers(recvb, pb_recv, z)
    for c in range(CH):
        for d in range(2):
            @pl.when(below[d] > 0)
            def _():
                s_wait(d, top, z if d == 0 else Q, c)

    step = 16

    def final(i, carry):
        at = pl.ds(pl.multiple_of(i * step, step), step)
        starts = tuple(base[j, at, :] + gin[z, j, at, :].astype(F32) + gin[Q, j, at, :].astype(F32)
                       for j in range(half))
        accs = sums(z, at, starts)
        for j in range(half):
            fgrad[j, at, :] = accs[j].astype(BF16)
        return carry

    lax.fori_loop(0, blk // step, final, 0)

    done(table.at[pl.ds(0, top)], t_send).wait_send()

    @pl.when(is_end)
    def _():
        done(sendf.at[pl.ds(0, top), pl.ds(0, plane - 1)], pf_send).wait_send()

    @pl.when(jnp.logical_not(is_end))
    def _():
        done(sendf.at[:, pl.ds(0, plane - 1)], pf_send).wait_send()
        done(sendx, x_send).wait_send()

    done(sendb.at[:, pl.ds(0, plane - 1)], pb_send).wait_send()
    for d in range(2):
        for k in range(top):
            @pl.when(below[d] == k)
            def _():
                done(gin.at[pl.ds(0, min(k + 1, hops))], lf_send.at[d]).wait_send()
                done(gin.at[pl.ds(0, top - k)], s_send.at[d]).wait_send()
    c_copy.wait_send()

    h_copy = remote(wall, wall, misc.at[10], misc.at[11], me, other)

    @pl.when(is_owner)
    def _():
        done(wchunk.at[pl.ds(0, doms - 1)], g_recv).wait_recv()

    @pl.when((col == 1) & jnp.logical_not(is_owner))
    def _():
        done(wchunk, g_recv).wait_recv()

    @pl.when(col == 1)
    def _():
        h_copy.start()

    @pl.when(col == 0)
    def _():
        h_copy.wait_recv()

    wgrad[...] = wall[...].astype(F32).reshape(wgrad.shape)

    @pl.when(is_owner)
    def _():
        done(wchunk.at[pl.ds(0, doms - 1)], r_send).wait_send()
        done(wpart.at[pl.ds(0, n - 1)], g_send).wait_send()

    @pl.when(jnp.logical_not(is_owner))
    def _():
        done(wchunk, r_send).wait_send()

    @pl.when(col == 1)
    def _():
        h_copy.wait_send()


def place(*refs):
    count = len(refs) // 2
    sem = refs[-1]
    writes = [pltpu.make_async_copy(a, b, sem.at[i]) for i, (a, b) in enumerate(zip(refs[:count], refs[count:-1]))]
    for write in writes:
        write.start()
    for write in writes:
        write.wait()


def finish(*arrays):
    return pl.pallas_call(
        place,
        out_shape=tuple(jax.ShapeDtypeStruct(a.shape, a.dtype) for a in arrays),
        in_specs=[pl.BlockSpec(memory_space=pltpu.VMEM)] * len(arrays),
        out_specs=(pl.BlockSpec(memory_space=pltpu.HBM),) * len(arrays),
        scratch_shapes=[pltpu.SemaphoreType.DMA((len(arrays),))],
        compiler_params=pltpu.CompilerParams(vmem_limit_bytes=4000000),
    )(*arrays)


def in_hbm(array):
    return pltpu.with_memory_space_constraint(array, pltpu.HBM)


def local(features, weight, cotangent, tile_values, tile_rows, tile_cols, tile_count, send_blocks):
    slots, blk, _ = tile_values.shape
    rows, width = features.shape
    width_out = cotangent.shape[1]
    half = rows // blk
    n = send_blocks.shape[1]
    plane = n // Q
    nodes = rows * lax.axis_size("col") * lax.axis_size("dom")
    scale = 1.0 / nodes**0.5
    bf = jnp.bfloat16
    doms = min(n // 2, width // 8)
    owners = (n // 4, doms)
    chunk = width // doms
    hbm = pl.BlockSpec(memory_space=pltpu.HBM)
    vmem = pl.BlockSpec(memory_space=pltpu.VMEM)
    smem = pl.BlockSpec(memory_space=pltpu.SMEM)
    sems = pltpu.SemaphoreType.DMA
    out, fgrad, wgrad = pl.pallas_call(
        functools.partial(kernel, scale, owners),
        out_shape=(
            jax.ShapeDtypeStruct((rows, width_out), bf),
            jax.ShapeDtypeStruct((half, blk, width), bf),
            jax.ShapeDtypeStruct((width, width_out), F32),
        ),
        in_specs=[hbm, hbm, smem] + [hbm] * 5,
        out_specs=(vmem, vmem, vmem),
        scratch_shapes=[
            pltpu.VMEM((half, blk, width), bf),
            pltpu.VMEM((width, width_out), bf),
            pltpu.VMEM((2 * rows, width_out), bf),
            pltpu.VMEM((slots, blk, blk), bf),
            pltpu.VMEM((Q, plane, blk, width), bf),
            pltpu.VMEM((Q, plane, blk, width), bf),
            pltpu.VMEM((Q, plane, blk, width), bf),
            pltpu.VMEM((Q, plane, blk, width), bf),
            pltpu.VMEM((Q + 1, half, blk, width), bf),
            pltpu.VMEM((slots + 1 + n, blk, width), F32),
            pltpu.VMEM((half, blk, width), F32),
            pltpu.VMEM((2 * half, blk, width), bf),
            pltpu.VMEM((half, blk, width), F32),
            pltpu.VMEM((half, blk, width), F32),
            pltpu.VMEM((plane, blk, width), bf),
            pltpu.VMEM((doms, chunk, width_out), bf),
            pltpu.VMEM((2 * n, chunk, width_out), bf),
            pltpu.VMEM((doms, chunk, width_out), bf),
            pltpu.SMEM((n,), jnp.int32),
            pltpu.SMEM((Q, n), jnp.int32),
            pltpu.SMEM((slots,), jnp.int32),
            pltpu.SMEM((slots,), jnp.int32),
            pltpu.SMEM((n,), jnp.int32),
        ] + [pltpu.VMEM((half, blk // CH, width), bf)] * (2 * (Q - 2) * CH) + [
            sems(()), sems(()), sems((2,)), sems((2,)), sems((2, Q, CH)),
            sems(()), sems((Q,)), sems(()), sems((Q,)),
            sems(()), sems(()), sems(()), sems(()), sems(()), sems((15,)),
        ],
        compiler_params=pltpu.CompilerParams(
            collective_id=0, has_side_effects=True, vmem_limit_bytes=min(67000000, 20000000 + 12 * n * blk * width)),
    )(in_hbm(tile_rows), in_hbm(tile_cols), tile_count, in_hbm(send_blocks.reshape(n)),
      in_hbm(features.reshape(half, blk, width)), in_hbm(weight), in_hbm(cotangent), in_hbm(tile_values))
    return finish(out, fgrad.reshape(rows, width), wgrad)


def solution(mesh):
    return jax.shard_map(
        local,
        mesh=mesh,
        in_specs=(
            P(("dom", "col"), None),
            P(),
            P(("dom", "col"), None),
            P(("dom", "col"), None, None),
            P(("dom", "col")),
            P(("dom", "col")),
            P(("dom", "col")),
            P(("dom", "col"), None),
        ),
        out_specs=(P(("dom", "col"), None), P(("dom", "col"), None), P()),
        check_vma=False,
    )
```

```python
import functools

import jax
import jax.numpy as jnp
from jax import lax
from jax.experimental import pallas as pl
from jax.experimental.pallas import tpu as pltpu
from jax.sharding import PartitionSpec as P

MESH = pl.DeviceIdType.MESH
F32 = jnp.float32
BF16 = jnp.bfloat16
Q = 4
CH = 2


def kernel(scale, owners, rows_hbm, cols_hbm, count_s, send_hbm, feat_hbm, weight_hbm, cot_hbm, tiles_hbm,
           out, fgrad, wgrad,
           feat, weight, cot, tiles, sendf, recvf, sendb, recvb, gin, buf, base, gh, psend, precv,
           sendx, wchunk, wpart, wall, tos, table,
           rows_s, cols_s, send_s, *rest):
    hops = Q - 2
    lines = rest[:2 * hops * CH]
    (t_send, t_recv, lf_send, s_send, l_recv, pf_send, pf_recv, pb_send, pb_recv,
     x_send, r_send, r_recv, g_send, g_recv, misc) = rest[2 * hops * CH:]
    slots = tiles.shape[0]
    half, blk, width = feat.shape
    plane = recvf.shape[1]
    n = Q * plane
    blocks = 2 * half
    top = Q - 1
    tall = blk // CH
    me = lax.axis_index("dom")
    col = lax.axis_index("col")
    other = 1 - col
    count = count_s[0]
    z, w = lax.div(me, plane), lax.rem(me, plane)
    below = (z, top - z)
    is_end = (z == 0) | (z == top)

    def remote(src, dst, s_sem, r_sem, dom, core):
        return pltpu.make_async_remote_copy(
            src_ref=src, dst_ref=dst, send_sem=s_sem, recv_sem=r_sem,
            device_id=(dom, core), device_id_type=MESH)

    def line(k):
        return lax.rem(z + k, Q)

    def peers(body):
        def step(k, carry):
            body(lax.rem(w + k, plane))
            return carry

        lax.fori_loop(1, plane, step, 0)

    feat_copy = pltpu.make_async_copy(feat_hbm, feat, misc.at[0])
    feat_copy.start()
    smalls = [pltpu.make_async_copy(a, b, misc.at[12 + i]) for i, (a, b) in enumerate(
        ((send_hbm, send_s), (rows_hbm, rows_s), (cols_hbm, cols_s)))]
    for small in smalls:
        small.start()
    barrier = pltpu.get_barrier_semaphore()

    def greet(dom, core):
        pl.semaphore_signal(barrier, inc=1, device_id=(dom, core), device_id_type=MESH)

    for k in range(1, Q):
        greet(line(k) * plane + w, col)
    peers(lambda peer: greet(z * plane + peer, col))
    greet(me, other)
    rows = half * blk
    cot_half = cot.at[pl.ds(pl.multiple_of(col * rows, rows), rows)]
    cot_copy = pltpu.make_async_copy(cot_hbm, cot_half, misc.at[1])
    cot_copy.start()
    weight_copy = pltpu.make_async_copy(weight_hbm, weight, misc.at[2])
    weight_copy.start()
    tile_copy = pltpu.make_async_copy(tiles_hbm, tiles, misc.at[3])
    tile_copy.start()

    gin[...] = jnp.zeros(gin.shape, gin.dtype)
    buf[0] = jnp.zeros((blk, width), F32)

    for small in smalls:
        small.wait()

    def keep(i, carry):
        table[z, i] = send_s[i]
        return carry

    lax.fori_loop(0, n, keep, 0)

    def part_of(c):
        return pl.ds(c * tall, tall)

    def pf_copy(s, peer, slot, at):
        return remote(sendf.at[s, peer, at], recvf.at[s, slot, at], pf_send, pf_recv.at[s],
                      z * plane + peer, col)

    def pb_copy(s, peer, slot):
        return remote(sendb.at[s, peer], recvb.at[s, slot], pb_send, pb_recv.at[s],
                      z * plane + peer, col)

    whole = pl.ds(0, blk)

    def done(ref, sem):
        return remote(ref, ref, sem, sem, me, other)

    def from_peers(buffer, sem, s):
        done(buffer.at[s, pl.ds(0, plane - 1)], sem.at[s]).wait_recv()

    def spread(source, s, at):
        def one(peer):
            sendf[s, peer, at, :] = source[table[s, z * plane + peer]]

        peers(one)
        peers(lambda peer: pf_copy(s, peer, w, at).start())
        recvf[s, w, at, :] = source[table[s, me]]

    def lf_copy(d, k, c):
        nxt = z + 1 if d == 0 else z - 1
        src = feat.at[:, part_of(c)] if k == 0 else lines[(d * hops + k - 1) * CH + c]
        return remote(src, lines[(d * hops + k) * CH + c], lf_send.at[d], l_recv.at[d, k, c],
                      nxt * plane + w, col)

    def s_copy(d, k, s, c):
        nxt = z + 1 if d == 0 else z - 1
        slot = s if d == 0 else jnp.where(s == nxt, Q, s)
        return remote(gin.at[s, :, part_of(c)], gin.at[slot, :, part_of(c)], s_send.at[d], l_recv.at[d, k + 1, c],
                      nxt * plane + w, col)

    def s_wait(d, k, slot, c):
        done(gin.at[slot, :, part_of(c)], l_recv.at[d, k, c]).wait_recv()

    def t_copy(k, slot):
        return remote(send_s, table.at[slot], t_send, t_recv, line(k) * plane + w, col)

    feat_copy.wait()
    pl.semaphore_wait(barrier, top + plane)

    for k in range(1, Q):
        t_copy(k, z).start()
    for c in range(CH):
        for d in range(2):
            @pl.when(below[d] < top)
            def _():
                lf_copy(d, 0, c).start()

    spread(feat, z, whole)
    cot_copy.wait()
    c_copy = remote(cot_half, cot_half, misc.at[4], misc.at[5], me, other)
    c_copy.start()

    def find(s, carry):
        found = jnp.int32(0)
        for t in range(slots):
            found = jnp.where((cols_s[t] == s + half) & (t < count), t + 1, found)
        tos[s] = found
        return carry

    lax.fori_loop(0, n, find, 0)
    weight_copy.wait()
    cot_other = cot.at[pl.ds(pl.multiple_of(other * rows, rows), rows)]
    remote(cot_other, cot_other, misc.at[4], misc.at[5], me, other).wait_recv()
    gh[...] = lax.dot_general(cot[...], weight[...], (((1,), (1,)), ((), ())),
                              preferred_element_type=F32).astype(BF16).reshape(gh.shape)
    tile_copy.wait()

    def back_term(slot):
        found = tos[slot]
        at = jnp.maximum(found - 1, 0)
        term = lax.dot_general(tiles[at], gh[rows_s[at]], (((0,), (0,)), ((), ())),
                               preferred_element_type=F32)
        return jnp.where(found > 0, term, 0.0).astype(BF16)

    def back_send(s):
        peers(lambda peer: pb_copy(s, peer, w).start())

    low_side = lax.div(z, Q // 2)
    far = top * (1 - low_side)
    near = 2 - low_side
    pair = z + 1 - 2 * lax.rem(z, 2)
    for i, s in enumerate((far, near, pair, z)):
        def fill(k, carry, s=s):
            peer = lax.rem(w + k, plane)
            sendb[s, peer] = back_term(s * plane + peer)
            return carry

        lax.fori_loop(0, plane, fill, 0, unroll=4)
        recvb[s, w] = sendb[s, w]
        if i == 0:
            back_send(s)

    def link(lasts, key, index):
        prev = jnp.int32(0)
        for r, last in enumerate(lasts):
            prev = jnp.where(key == r, last, prev)
        return prev, tuple(jnp.where(key == r, index, last) for r, last in enumerate(lasts))

    def own_back(t, lasts):
        key = jnp.where(t < count, cols_s[t], -1)
        prev, lasts = link(lasts, key, t + 1)
        term = lax.dot_general(tiles[t], gh[rows_s[t]], (((0,), (0,)), ((), ())),
                               preferred_element_type=F32)
        buf[t + 1] = buf[prev] + term
        return lasts

    unroll = 4 if slots % 4 == 0 else 1

    def own_fwd(t, lasts):
        source = cols_s[t]
        key = jnp.where((t < count) & (source < half), rows_s[t], -1)
        prev, lasts = link(lasts, key, t + 1)
        term = jnp.dot(tiles[t], feat[jnp.minimum(source, half - 1)], preferred_element_type=F32)
        buf[t + 1] = buf[prev] + term
        return lasts

    def slot_group(g, lasts):
        if g == 0:
            s = z
        else:
            zm = z + low_side * (top - 2 * z)
            rel = g - 1 + jnp.where(g <= zm, 0, 1)
            s = rel + low_side * (top - 2 * rel)
        if g < top:
            from_peers(recvf, pf_recv, s)
        else:
            @pl.when(is_end)
            def _():
                done(recvf.at[s], pf_recv.at[s]).wait_recv()

            @pl.when(jnp.logical_not(is_end))
            def _():
                from_peers(recvf, pf_recv, s)


        def step(k, lasts):
            slot = lax.rem(w + k, plane)
            found = tos[s * plane + slot]
            at = jnp.maximum(found - 1, 0)
            key = jnp.where(found > 0, rows_s[at], -1)
            index = slots + 1 + g * plane + k
            prev, lasts = link(lasts, key, index)
            term = jnp.dot(tiles[at], recvf[s, slot], preferred_element_type=F32)
            buf[index] = buf[prev] + term
            return lasts

        return lax.fori_loop(0, plane, step, lasts, unroll=4)

    def sums(s, at, starts):
        def add(slot, accs):
            value = recvb[s, slot, at, :].astype(F32)
            home = table[s, z * plane + slot]
            return tuple(acc + jnp.where(home == j, value, 0.0) for j, acc in enumerate(accs))

        return lax.fori_loop(0, plane, add, starts, unroll=4)

    def sum_of(k, d):
        rel = top - (k - below[d])
        return rel if d == 0 else top - rel

    def feat_of(k, d):
        rel = below[d] - 1 - k
        return rel if d == 0 else top - rel

    def reach(d, source, s, at):
        nxt = (z + 1 if d == 0 else z - 1) * plane

        def one(k, carry):
            peer = lax.rem(w + k, plane)
            sendx[peer, at, :] = source[table[s, nxt + peer]]
            return carry

        def go(k, carry):
            peer = lax.rem(w + k, plane)
            remote(sendx.at[peer, at], recvf.at[s, w, at], x_send, pf_recv.at[s], nxt + peer, col).start()
            return carry

        lax.fori_loop(0, plane, one, 0)
        lax.fori_loop(0, plane, go, 0)

    def feats(k):
        for c in range(CH):
            for d in range(2):
                @pl.when(k < below[d])
                def _():
                    lf_copy(d, k, c).wait_recv()

                    @pl.when(below[d] < top)
                    def _():
                        if k + 1 < hops:
                            lf_copy(d, k + 1, c).start()
                        else:
                            reach(d, lines[(d * hops + k) * CH + c], feat_of(k, d), part_of(c))

            for d in range(2):
                @pl.when(k < below[d])
                def _():
                    spread(lines[(d * hops + k) * CH + c], feat_of(k, d), part_of(c))

    def grads(k):
        for d in range(2):
            @pl.when(below[d] <= k)
            def _():
                from_peers(recvb, pb_recv, sum_of(k, d))

        step = tall // 2
        for c in range(CH):
            for d in range(2):
                @pl.when(below[d] <= k)
                def _():
                    s = sum_of(k, d)

                    @pl.when(below[d] > 0)
                    def _():
                        s_wait(d, k, s, c)

                    def some(i, carry):
                        at = pl.ds(pl.multiple_of(c * tall + i * step, step), step)
                        accs = sums(s, at, tuple(gin[s, j, at, :].astype(F32) for j in range(half)))
                        for j in range(half):
                            gin[s, j, at, :] = accs[j].astype(BF16)
                        return carry

                    lax.fori_loop(0, tall // step, some, 0)
                    s_copy(d, k, s, c).start()

    lasts = lax.fori_loop(0, slots, own_back, (jnp.int32(0),) * half, unroll=unroll)
    for j in range(half):
        base[j] = buf[lasts[j]]
    done(table.at[pl.ds(0, top)], t_recv).wait_recv()

    feats(0)
    back_send(near)
    grads(0)
    feats(1)
    grads(1)

    back_send(pair)

    @pl.when(jnp.logical_not(is_end))
    def _():
        back_send(z)

    lasts = slot_group(0, (jnp.int32(0),) * blocks)
    lasts = lax.fori_loop(0, slots, own_fwd, lasts, unroll=unroll)
    for g in range(1, Q):
        lasts = slot_group(g, lasts)

    for r in range(blocks):
        gh[r] = buf[lasts[r]].astype(BF16)
    term = lax.dot_general(gh[...].reshape(cot.shape), cot[...], (((0,), (0,)), ((), ())),
                           preferred_element_type=F32) * jnp.float32(scale)
    wchunk[...] = term.astype(BF16).reshape(wchunk.shape)

    first, doms = owners
    mine = me - first
    is_owner = (col == 1) & (me >= first) & (me < first + doms)

    def others(limit, start, skip, body):
        def step(k, carry):
            at = lax.rem(start + k, limit)

            @pl.when(at != skip)
            def _():
                body(at)
            return carry

        lax.fori_loop(0, limit, step, 0)

    flat = 2 * me + col
    keep_own = jnp.where(is_owner, mine, doms)
    others(doms, lax.rem(me, doms), keep_own,
           lambda i: remote(wchunk.at[i], wpart.at[flat], r_send, r_recv, first + i, 1).start())

    for j in range(half):
        psend[j] = buf[jnp.where(col == 0, lasts[half + j], lasts[j])]
    p_copy = remote(psend, precv, misc.at[6], misc.at[7], me, other)
    p_copy.start()

    @pl.when(is_end)
    def _():
        back_send(z)

    grads(2)

    p_copy.wait()
    for j in range(half):
        whose = buf[jnp.where(col == 0, lasts[j], lasts[half + j])]
        hidden = (whose + precv[j]).astype(BF16)
        out[pl.ds(j * blk, blk), :] = jnp.dot(hidden, weight[...], preferred_element_type=F32).astype(BF16)

    @pl.when(is_owner)
    def _():
        wpart[flat] = wchunk[mine]
        done(wpart.at[pl.ds(0, 2 * n - 1)], r_recv).wait_recv()
        total = lax.fori_loop(0, 2 * n, lambda f, acc: acc + wpart[f].astype(F32),
                              jnp.zeros(wpart.shape[1:], F32), unroll=4)
        wall[mine] = total.astype(BF16)
        others(n, me, me,
               lambda f: remote(wall.at[mine], wall.at[mine], g_send, g_recv, f, 1).start())

    from_peers(recvb, pb_recv, z)
    for c in range(CH):
        for d in range(2):
            @pl.when(below[d] > 0)
            def _():
                s_wait(d, top, z if d == 0 else Q, c)

    step = 16

    def final(i, carry):
        at = pl.ds(pl.multiple_of(i * step, step), step)
        starts = tuple(base[j, at, :] + gin[z, j, at, :].astype(F32) + gin[Q, j, at, :].astype(F32)
                       for j in range(half))
        accs = sums(z, at, starts)
        for j in range(half):
            fgrad[j, at, :] = accs[j].astype(BF16)
        return carry

    lax.fori_loop(0, blk // step, final, 0)

    done(table.at[pl.ds(0, top)], t_send).wait_send()

    @pl.when(is_end)
    def _():
        done(sendf.at[pl.ds(0, top), pl.ds(0, plane - 1)], pf_send).wait_send()

    @pl.when(jnp.logical_not(is_end))
    def _():
        done(sendf.at[:, pl.ds(0, plane - 1)], pf_send).wait_send()
        done(sendx, x_send).wait_send()

    done(sendb.at[:, pl.ds(0, plane - 1)], pb_send).wait_send()
    for d in range(2):
        for k in range(top):
            @pl.when(below[d] == k)
            def _():
                done(gin.at[pl.ds(0, min(k + 1, hops))], lf_send.at[d]).wait_send()
                done(gin.at[pl.ds(0, top - k)], s_send.at[d]).wait_send()
    c_copy.wait_send()

    h_copy = remote(wall, wall, misc.at[10], misc.at[11], me, other)

    @pl.when(is_owner)
    def _():
        done(wchunk.at[pl.ds(0, doms - 1)], g_recv).wait_recv()

    @pl.when((col == 1) & jnp.logical_not(is_owner))
    def _():
        done(wchunk, g_recv).wait_recv()

    @pl.when(col == 1)
    def _():
        h_copy.start()

    @pl.when(col == 0)
    def _():
        h_copy.wait_recv()

    wgrad[...] = wall[...].astype(F32).reshape(wgrad.shape)

    @pl.when(is_owner)
    def _():
        done(wchunk.at[pl.ds(0, doms - 1)], r_send).wait_send()
        done(wpart.at[pl.ds(0, n - 1)], g_send).wait_send()

    @pl.when(jnp.logical_not(is_owner))
    def _():
        done(wchunk, r_send).wait_send()

    @pl.when(col == 1)
    def _():
        h_copy.wait_send()


def place(*refs):
    count = len(refs) // 2
    sem = refs[-1]
    writes = [pltpu.make_async_copy(a, b, sem.at[i]) for i, (a, b) in enumerate(zip(refs[:count], refs[count:-1]))]
    for write in writes:
        write.start()
    for write in writes:
        write.wait()


def finish(*arrays):
    return pl.pallas_call(
        place,
        out_shape=tuple(jax.ShapeDtypeStruct(a.shape, a.dtype) for a in arrays),
        in_specs=[pl.BlockSpec(memory_space=pltpu.VMEM)] * len(arrays),
        out_specs=(pl.BlockSpec(memory_space=pltpu.HBM),) * len(arrays),
        scratch_shapes=[pltpu.SemaphoreType.DMA((len(arrays),))],
        compiler_params=pltpu.CompilerParams(vmem_limit_bytes=4000000),
    )(*arrays)


def in_hbm(array):
    return pltpu.with_memory_space_constraint(array, pltpu.HBM)


def local(features, weight, cotangent, tile_values, tile_rows, tile_cols, tile_count, send_blocks):
    slots, blk, _ = tile_values.shape
    rows, width = features.shape
    width_out = cotangent.shape[1]
    half = rows // blk
    n = send_blocks.shape[1]
    plane = n // Q
    nodes = rows * lax.axis_size("col") * lax.axis_size("dom")
    scale = 1.0 / nodes**0.5
    bf = jnp.bfloat16
    doms = min(n // 2, width // 8)
    owners = (n // 4, doms)
    chunk = width // doms
    hbm = pl.BlockSpec(memory_space=pltpu.HBM)
    vmem = pl.BlockSpec(memory_space=pltpu.VMEM)
    smem = pl.BlockSpec(memory_space=pltpu.SMEM)
    sems = pltpu.SemaphoreType.DMA
    out, fgrad, wgrad = pl.pallas_call(
        functools.partial(kernel, scale, owners),
        out_shape=(
            jax.ShapeDtypeStruct((rows, width_out), bf),
            jax.ShapeDtypeStruct((half, blk, width), bf),
            jax.ShapeDtypeStruct((width, width_out), F32),
        ),
        in_specs=[hbm, hbm, smem] + [hbm] * 5,
        out_specs=(vmem, vmem, vmem),
        scratch_shapes=[
            pltpu.VMEM((half, blk, width), bf),
            pltpu.VMEM((width, width_out), bf),
            pltpu.VMEM((2 * rows, width_out), bf),
            pltpu.VMEM((slots, blk, blk), bf),
            pltpu.VMEM((Q, plane, blk, width), bf),
            pltpu.VMEM((Q, plane, blk, width), bf),
            pltpu.VMEM((Q, plane, blk, width), bf),
            pltpu.VMEM((Q, plane, blk, width), bf),
            pltpu.VMEM((Q + 1, half, blk, width), bf),
            pltpu.VMEM((slots + 1 + n, blk, width), F32),
            pltpu.VMEM((half, blk, width), F32),
            pltpu.VMEM((2 * half, blk, width), bf),
            pltpu.VMEM((half, blk, width), F32),
            pltpu.VMEM((half, blk, width), F32),
            pltpu.VMEM((plane, blk, width), bf),
            pltpu.VMEM((doms, chunk, width_out), bf),
            pltpu.VMEM((2 * n, chunk, width_out), bf),
            pltpu.VMEM((doms, chunk, width_out), bf),
            pltpu.SMEM((n,), jnp.int32),
            pltpu.SMEM((Q, n), jnp.int32),
            pltpu.SMEM((slots,), jnp.int32),
            pltpu.SMEM((slots,), jnp.int32),
            pltpu.SMEM((n,), jnp.int32),
        ] + [pltpu.VMEM((half, blk // CH, width), bf)] * (2 * (Q - 2) * CH) + [
            sems(()), sems(()), sems((2,)), sems((2,)), sems((2, Q, CH)),
            sems(()), sems((Q,)), sems(()), sems((Q,)),
            sems(()), sems(()), sems(()), sems(()), sems(()), sems((15,)),
        ],
        compiler_params=pltpu.CompilerParams(
            collective_id=0, has_side_effects=True, vmem_limit_bytes=min(67000000, 20000000 + 12 * n * blk * width)),
    )(in_hbm(tile_rows), in_hbm(tile_cols), tile_count, in_hbm(send_blocks.reshape(n)),
      in_hbm(features.reshape(half, blk, width)), in_hbm(weight), in_hbm(cotangent), in_hbm(tile_values))
    return finish(out, fgrad.reshape(rows, width), wgrad)


def solution(mesh):
    return jax.shard_map(
        local,
        mesh=mesh,
        in_specs=(
            P(("dom", "col"), None),
            P(),
            P(("dom", "col"), None),
            P(("dom", "col"), None, None),
            P(("dom", "col")),
            P(("dom", "col")),
            P(("dom", "col")),
            P(("dom", "col"), None),
        ),
        out_specs=(P(("dom", "col"), None), P(("dom", "col"), None), P()),
        check_vma=False,
    )
```

```python
import functools

import jax
import jax.numpy as jnp
from jax import lax
from jax.experimental import pallas as pl
from jax.experimental.pallas import tpu as pltpu
from jax.sharding import PartitionSpec as P

MESH = pl.DeviceIdType.MESH
F32 = jnp.float32
BF16 = jnp.bfloat16
Q = 4
CH = 2


def kernel(scale, owners, rows_hbm, cols_hbm, count_s, send_hbm, feat_hbm, weight_hbm, cot_hbm, tiles_hbm,
           out, fgrad, wgrad,
           feat, weight, cot, tiles, sendf, recvf, sendb, recvb, gin, buf, base, gh, psend, precv,
           sendx, wchunk, wpart, wall, tos, table,
           rows_s, cols_s, send_s, *rest):
    hops = Q - 2
    lines = rest[:2 * hops * CH]
    (t_send, t_recv, lf_send, s_send, l_recv, pf_send, pf_recv, pb_send, pb_recv,
     x_send, r_send, r_recv, g_send, g_recv, misc) = rest[2 * hops * CH:]
    slots = tiles.shape[0]
    half, blk, width = feat.shape
    plane = recvf.shape[1]
    n = Q * plane
    blocks = 2 * half
    top = Q - 1
    tall = blk // CH
    me = lax.axis_index("dom")
    col = lax.axis_index("col")
    other = 1 - col
    count = count_s[0]
    z, w = lax.div(me, plane), lax.rem(me, plane)
    below = (z, top - z)
    is_end = (z == 0) | (z == top)

    def remote(src, dst, s_sem, r_sem, dom, core):
        return pltpu.make_async_remote_copy(
            src_ref=src, dst_ref=dst, send_sem=s_sem, recv_sem=r_sem,
            device_id=(dom, core), device_id_type=MESH)

    def line(k):
        return lax.rem(z + k, Q)

    def peers(body):
        def step(k, carry):
            body(lax.rem(w + k, plane))
            return carry

        lax.fori_loop(1, plane, step, 0)

    feat_copy = pltpu.make_async_copy(feat_hbm, feat, misc.at[0])
    feat_copy.start()
    smalls = [pltpu.make_async_copy(a, b, misc.at[12 + i]) for i, (a, b) in enumerate(
        ((send_hbm, send_s), (rows_hbm, rows_s), (cols_hbm, cols_s)))]
    for small in smalls:
        small.start()
    barrier = pltpu.get_barrier_semaphore()

    def greet(dom, core):
        pl.semaphore_signal(barrier, inc=1, device_id=(dom, core), device_id_type=MESH)

    for k in range(1, Q):
        greet(line(k) * plane + w, col)
    peers(lambda peer: greet(z * plane + peer, col))
    greet(me, other)
    rows = half * blk
    cot_half = cot.at[pl.ds(pl.multiple_of(col * rows, rows), rows)]
    cot_copy = pltpu.make_async_copy(cot_hbm, cot_half, misc.at[1])
    cot_copy.start()
    weight_copy = pltpu.make_async_copy(weight_hbm, weight, misc.at[2])
    weight_copy.start()
    tile_copy = pltpu.make_async_copy(tiles_hbm, tiles, misc.at[3])
    tile_copy.start()

    gin[...] = jnp.zeros(gin.shape, gin.dtype)
    buf[0] = jnp.zeros((blk, width), F32)

    for small in smalls:
        small.wait()

    def keep(i, carry):
        table[z, i] = send_s[i]
        return carry

    lax.fori_loop(0, n, keep, 0)

    def part_of(c):
        return pl.ds(c * tall, tall)

    def pf_copy(s, peer, slot, at):
        return remote(sendf.at[s, peer, at], recvf.at[s, slot, at], pf_send, pf_recv.at[s],
                      z * plane + peer, col)

    def pb_copy(s, peer, slot):
        return remote(sendb.at[s, peer], recvb.at[s, slot], pb_send, pb_recv.at[s],
                      z * plane + peer, col)

    whole = pl.ds(0, blk)

    def done(ref, sem):
        return remote(ref, ref, sem, sem, me, other)

    def from_peers(buffer, sem, s):
        done(buffer.at[s, pl.ds(0, plane - 1)], sem.at[s]).wait_recv()

    def spread(source, s, at):
        def one(peer):
            sendf[s, peer, at, :] = source[table[s, z * plane + peer]]

        peers(one)
        peers(lambda peer: pf_copy(s, peer, w, at).start())
        recvf[s, w, at, :] = source[table[s, me]]

    def lf_copy(d, k, c):
        nxt = z + 1 if d == 0 else z - 1
        src = feat.at[:, part_of(c)] if k == 0 else lines[(d * hops + k - 1) * CH + c]
        return remote(src, lines[(d * hops + k) * CH + c], lf_send.at[d], l_recv.at[d, k, c],
                      nxt * plane + w, col)

    def s_copy(d, k, s, c):
        nxt = z + 1 if d == 0 else z - 1
        slot = s if d == 0 else jnp.where(s == nxt, Q, s)
        return remote(gin.at[s, :, part_of(c)], gin.at[slot, :, part_of(c)], s_send.at[d], l_recv.at[d, k + 1, c],
                      nxt * plane + w, col)

    def s_wait(d, k, slot, c):
        done(gin.at[slot, :, part_of(c)], l_recv.at[d, k, c]).wait_recv()

    def t_copy(k, slot):
        return remote(send_s, table.at[slot], t_send, t_recv, line(k) * plane + w, col)

    feat_copy.wait()
    pl.semaphore_wait(barrier, top + plane)

    for k in range(1, Q):
        t_copy(k, z).start()
    for c in range(CH):
        for d in range(2):
            @pl.when(below[d] < top)
            def _():
                lf_copy(d, 0, c).start()

    spread(feat, z, whole)
    cot_copy.wait()
    c_copy = remote(cot_half, cot_half, misc.at[4], misc.at[5], me, other)
    c_copy.start()

    def find(s, carry):
        found = jnp.int32(0)
        for t in range(slots):
            found = jnp.where((cols_s[t] == s + half) & (t < count), t + 1, found)
        tos[s] = found
        return carry

    lax.fori_loop(0, n, find, 0)
    weight_copy.wait()
    cot_other = cot.at[pl.ds(pl.multiple_of(other * rows, rows), rows)]
    remote(cot_other, cot_other, misc.at[4], misc.at[5], me, other).wait_recv()
    gh[...] = lax.dot_general(cot[...], weight[...], (((1,), (1,)), ((), ())),
                              preferred_element_type=F32).astype(BF16).reshape(gh.shape)
    tile_copy.wait()

    def back_term(slot):
        found = tos[slot]
        at = jnp.maximum(found - 1, 0)
        term = lax.dot_general(tiles[at], gh[rows_s[at]], (((0,), (0,)), ((), ())),
                               preferred_element_type=F32)
        return jnp.where(found > 0, term, 0.0).astype(BF16)

    def back_send(s):
        peers(lambda peer: pb_copy(s, peer, w).start())

    low_side = lax.div(z, Q // 2)
    far = top * (1 - low_side)
    near = 2 - low_side
    pair = z + 1 - 2 * lax.rem(z, 2)
    for i, s in enumerate((far, near, pair, z)):
        def fill(k, carry, s=s):
            peer = lax.rem(w + k, plane)
            sendb[s, peer] = back_term(s * plane + peer)
            return carry

        lax.fori_loop(0, plane, fill, 0, unroll=4)
        recvb[s, w] = sendb[s, w]
        if i == 0:
            back_send(s)

    def link(lasts, key, index):
        prev = jnp.int32(0)
        for r, last in enumerate(lasts):
            prev = jnp.where(key == r, last, prev)
        return prev, tuple(jnp.where(key == r, index, last) for r, last in enumerate(lasts))

    def own_back(t, lasts):
        key = jnp.where(t < count, cols_s[t], -1)
        prev, lasts = link(lasts, key, t + 1)
        term = lax.dot_general(tiles[t], gh[rows_s[t]], (((0,), (0,)), ((), ())),
                               preferred_element_type=F32)
        buf[t + 1] = buf[prev] + term
        return lasts

    unroll = 4 if slots % 4 == 0 else 1

    def own_fwd(t, lasts):
        source = cols_s[t]
        key = jnp.where((t < count) & (source < half), rows_s[t], -1)
        prev, lasts = link(lasts, key, t + 1)
        term = jnp.dot(tiles[t], feat[jnp.minimum(source, half - 1)], preferred_element_type=F32)
        buf[t + 1] = buf[prev] + term
        return lasts

    def slot_group(g, lasts):
        if g == 0:
            s = z
        else:
            zm = z + low_side * (top - 2 * z)
            rel = g - 1 + jnp.where(g <= zm, 0, 1)
            s = rel + low_side * (top - 2 * rel)
        if g < top:
            from_peers(recvf, pf_recv, s)
        else:
            @pl.when(is_end)
            def _():
                done(recvf.at[s], pf_recv.at[s]).wait_recv()

            @pl.when(jnp.logical_not(is_end))
            def _():
                from_peers(recvf, pf_recv, s)


        def step(k, lasts):
            slot = lax.rem(w + k, plane)
            found = tos[s * plane + slot]
            at = jnp.maximum(found - 1, 0)
            key = jnp.where(found > 0, rows_s[at], -1)
            index = slots + 1 + g * plane + k
            prev, lasts = link(lasts, key, index)
            term = jnp.dot(tiles[at], recvf[s, slot], preferred_element_type=F32)
            buf[index] = buf[prev] + term
            return lasts

        return lax.fori_loop(0, plane, step, lasts, unroll=4)

    def sums(s, at, starts):
        def add(slot, accs):
            value = recvb[s, slot, at, :].astype(F32)
            home = table[s, z * plane + slot]
            return tuple(acc + jnp.where(home == j, value, 0.0) for j, acc in enumerate(accs))

        return lax.fori_loop(0, plane, add, starts, unroll=4)

    def sum_of(k, d):
        rel = top - (k - below[d])
        return rel if d == 0 else top - rel

    def feat_of(k, d):
        rel = below[d] - 1 - k
        return rel if d == 0 else top - rel

    def reach(d, source, s, at):
        nxt = (z + 1 if d == 0 else z - 1) * plane

        def one(k, carry):
            peer = lax.rem(w + k, plane)
            sendx[peer, at, :] = source[table[s, nxt + peer]]
            return carry

        def go(k, carry):
            peer = lax.rem(w + k, plane)
            remote(sendx.at[peer, at], recvf.at[s, w, at], x_send, pf_recv.at[s], nxt + peer, col).start()
            return carry

        lax.fori_loop(0, plane, one, 0)
        lax.fori_loop(0, plane, go, 0)

    def feats(k):
        for c in range(CH):
            for d in range(2):
                @pl.when(k < below[d])
                def _():
                    lf_copy(d, k, c).wait_recv()

                    @pl.when(below[d] < top)
                    def _():
                        if k + 1 < hops:
                            lf_copy(d, k + 1, c).start()
                        else:
                            reach(d, lines[(d * hops + k) * CH + c], feat_of(k, d), part_of(c))

            for d in range(2):
                @pl.when(k < below[d])
                def _():
                    spread(lines[(d * hops + k) * CH + c], feat_of(k, d), part_of(c))

    def grads(k):
        for d in range(2):
            @pl.when(below[d] <= k)
            def _():
                from_peers(recvb, pb_recv, sum_of(k, d))

        step = tall // 2
        for c in range(CH):
            for d in range(2):
                @pl.when(below[d] <= k)
                def _():
                    s = sum_of(k, d)

                    @pl.when(below[d] > 0)
                    def _():
                        s_wait(d, k, s, c)

                    def some(i, carry):
                        at = pl.ds(pl.multiple_of(c * tall + i * step, step), step)
                        accs = sums(s, at, tuple(gin[s, j, at, :].astype(F32) for j in range(half)))
                        for j in range(half):
                            gin[s, j, at, :] = accs[j].astype(BF16)
                        return carry

                    lax.fori_loop(0, tall // step, some, 0)
                    s_copy(d, k, s, c).start()

    lasts = lax.fori_loop(0, slots, own_back, (jnp.int32(0),) * half, unroll=unroll)
    for j in range(half):
        base[j] = buf[lasts[j]]
    done(table.at[pl.ds(0, top)], t_recv).wait_recv()

    feats(0)
    back_send(near)
    grads(0)
    feats(1)
    grads(1)

    back_send(pair)

    @pl.when(jnp.logical_not(is_end))
    def _():
        back_send(z)

    lasts = slot_group(0, (jnp.int32(0),) * blocks)
    lasts = lax.fori_loop(0, slots, own_fwd, lasts, unroll=unroll)
    for g in range(1, Q):
        lasts = slot_group(g, lasts)

    for r in range(blocks):
        gh[r] = buf[lasts[r]].astype(BF16)
    term = lax.dot_general(gh[...].reshape(cot.shape), cot[...], (((0,), (0,)), ((), ())),
                           preferred_element_type=F32) * jnp.float32(scale)
    wchunk[...] = term.astype(BF16).reshape(wchunk.shape)

    first, doms = owners
    mine = me - first
    is_owner = (col == 1) & (me >= first) & (me < first + doms)

    def others(limit, start, skip, body):
        def step(k, carry):
            at = lax.rem(start + k, limit)

            @pl.when(at != skip)
            def _():
                body(at)
            return carry

        lax.fori_loop(0, limit, step, 0)

    flat = 2 * me + col
    keep_own = jnp.where(is_owner, mine, doms)
    others(doms, lax.rem(me + doms // 2, doms), keep_own,
           lambda i: remote(wchunk.at[i], wpart.at[flat], r_send, r_recv, first + i, 1).start())

    for j in range(half):
        psend[j] = buf[jnp.where(col == 0, lasts[half + j], lasts[j])]
    p_copy = remote(psend, precv, misc.at[6], misc.at[7], me, other)
    p_copy.start()

    @pl.when(is_end)
    def _():
        back_send(z)

    grads(2)

    p_copy.wait()
    for j in range(half):
        whose = buf[jnp.where(col == 0, lasts[j], lasts[half + j])]
        hidden = (whose + precv[j]).astype(BF16)
        out[pl.ds(j * blk, blk), :] = jnp.dot(hidden, weight[...], preferred_element_type=F32).astype(BF16)

    @pl.when(is_owner)
    def _():
        wpart[flat] = wchunk[mine]
        done(wpart.at[pl.ds(0, 2 * n - 1)], r_recv).wait_recv()
        total = lax.fori_loop(0, 2 * n, lambda f, acc: acc + wpart[f].astype(F32),
                              jnp.zeros(wpart.shape[1:], F32), unroll=4)
        wall[mine] = total.astype(BF16)
        others(n, me, me,
               lambda f: remote(wall.at[mine], wall.at[mine], g_send, g_recv, f, 1).start())

    from_peers(recvb, pb_recv, z)
    for c in range(CH):
        for d in range(2):
            @pl.when(below[d] > 0)
            def _():
                s_wait(d, top, z if d == 0 else Q, c)

    step = 16

    def final(i, carry):
        at = pl.ds(pl.multiple_of(i * step, step), step)
        starts = tuple(base[j, at, :] + gin[z, j, at, :].astype(F32) + gin[Q, j, at, :].astype(F32)
                       for j in range(half))
        accs = sums(z, at, starts)
        for j in range(half):
            fgrad[j, at, :] = accs[j].astype(BF16)
        return carry

    lax.fori_loop(0, blk // step, final, 0)

    done(table.at[pl.ds(0, top)], t_send).wait_send()

    @pl.when(is_end)
    def _():
        done(sendf.at[pl.ds(0, top), pl.ds(0, plane - 1)], pf_send).wait_send()

    @pl.when(jnp.logical_not(is_end))
    def _():
        done(sendf.at[:, pl.ds(0, plane - 1)], pf_send).wait_send()
        done(sendx, x_send).wait_send()

    done(sendb.at[:, pl.ds(0, plane - 1)], pb_send).wait_send()
    for d in range(2):
        for k in range(top):
            @pl.when(below[d] == k)
            def _():
                done(gin.at[pl.ds(0, min(k + 1, hops))], lf_send.at[d]).wait_send()
                done(gin.at[pl.ds(0, top - k)], s_send.at[d]).wait_send()
    c_copy.wait_send()

    h_copy = remote(wall, wall, misc.at[10], misc.at[11], me, other)

    @pl.when(is_owner)
    def _():
        done(wchunk.at[pl.ds(0, doms - 1)], g_recv).wait_recv()

    @pl.when((col == 1) & jnp.logical_not(is_owner))
    def _():
        done(wchunk, g_recv).wait_recv()

    @pl.when(col == 1)
    def _():
        h_copy.start()

    @pl.when(col == 0)
    def _():
        h_copy.wait_recv()

    wgrad[...] = wall[...].astype(F32).reshape(wgrad.shape)

    @pl.when(is_owner)
    def _():
        done(wchunk.at[pl.ds(0, doms - 1)], r_send).wait_send()
        done(wpart.at[pl.ds(0, n - 1)], g_send).wait_send()

    @pl.when(jnp.logical_not(is_owner))
    def _():
        done(wchunk, r_send).wait_send()

    @pl.when(col == 1)
    def _():
        h_copy.wait_send()


def place(*refs):
    count = len(refs) // 2
    sem = refs[-1]
    writes = [pltpu.make_async_copy(a, b, sem.at[i]) for i, (a, b) in enumerate(zip(refs[:count], refs[count:-1]))]
    for write in writes:
        write.start()
    for write in writes:
        write.wait()


def finish(*arrays):
    return pl.pallas_call(
        place,
        out_shape=tuple(jax.ShapeDtypeStruct(a.shape, a.dtype) for a in arrays),
        in_specs=[pl.BlockSpec(memory_space=pltpu.VMEM)] * len(arrays),
        out_specs=(pl.BlockSpec(memory_space=pltpu.HBM),) * len(arrays),
        scratch_shapes=[pltpu.SemaphoreType.DMA((len(arrays),))],
        compiler_params=pltpu.CompilerParams(vmem_limit_bytes=4000000),
    )(*arrays)


def in_hbm(array):
    return pltpu.with_memory_space_constraint(array, pltpu.HBM)


def local(features, weight, cotangent, tile_values, tile_rows, tile_cols, tile_count, send_blocks):
    slots, blk, _ = tile_values.shape
    rows, width = features.shape
    width_out = cotangent.shape[1]
    half = rows // blk
    n = send_blocks.shape[1]
    plane = n // Q
    nodes = rows * lax.axis_size("col") * lax.axis_size("dom")
    scale = 1.0 / nodes**0.5
    bf = jnp.bfloat16
    doms = min(n // 2, width // 8)
    owners = (n // 4, doms)
    chunk = width // doms
    hbm = pl.BlockSpec(memory_space=pltpu.HBM)
    vmem = pl.BlockSpec(memory_space=pltpu.VMEM)
    smem = pl.BlockSpec(memory_space=pltpu.SMEM)
    sems = pltpu.SemaphoreType.DMA
    out, fgrad, wgrad = pl.pallas_call(
        functools.partial(kernel, scale, owners),
        out_shape=(
            jax.ShapeDtypeStruct((rows, width_out), bf),
            jax.ShapeDtypeStruct((half, blk, width), bf),
            jax.ShapeDtypeStruct((width, width_out), F32),
        ),
        in_specs=[hbm, hbm, smem] + [hbm] * 5,
        out_specs=(vmem, vmem, vmem),
        scratch_shapes=[
            pltpu.VMEM((half, blk, width), bf),
            pltpu.VMEM((width, width_out), bf),
            pltpu.VMEM((2 * rows, width_out), bf),
            pltpu.VMEM((slots, blk, blk), bf),
            pltpu.VMEM((Q, plane, blk, width), bf),
            pltpu.VMEM((Q, plane, blk, width), bf),
            pltpu.VMEM((Q, plane, blk, width), bf),
            pltpu.VMEM((Q, plane, blk, width), bf),
            pltpu.VMEM((Q + 1, half, blk, width), bf),
            pltpu.VMEM((slots + 1 + n, blk, width), F32),
            pltpu.VMEM((half, blk, width), F32),
            pltpu.VMEM((2 * half, blk, width), bf),
            pltpu.VMEM((half, blk, width), F32),
            pltpu.VMEM((half, blk, width), F32),
            pltpu.VMEM((plane, blk, width), bf),
            pltpu.VMEM((doms, chunk, width_out), bf),
            pltpu.VMEM((2 * n, chunk, width_out), bf),
            pltpu.VMEM((doms, chunk, width_out), bf),
            pltpu.SMEM((n,), jnp.int32),
            pltpu.SMEM((Q, n), jnp.int32),
            pltpu.SMEM((slots,), jnp.int32),
            pltpu.SMEM((slots,), jnp.int32),
            pltpu.SMEM((n,), jnp.int32),
        ] + [pltpu.VMEM((half, blk // CH, width), bf)] * (2 * (Q - 2) * CH) + [
            sems(()), sems(()), sems((2,)), sems((2,)), sems((2, Q, CH)),
            sems(()), sems((Q,)), sems(()), sems((Q,)),
            sems(()), sems(()), sems(()), sems(()), sems(()), sems((15,)),
        ],
        compiler_params=pltpu.CompilerParams(
            collective_id=0, has_side_effects=True, vmem_limit_bytes=min(67000000, 20000000 + 12 * n * blk * width)),
    )(in_hbm(tile_rows), in_hbm(tile_cols), tile_count, in_hbm(send_blocks.reshape(n)),
      in_hbm(features.reshape(half, blk, width)), in_hbm(weight), in_hbm(cotangent), in_hbm(tile_values))
    return finish(out, fgrad.reshape(rows, width), wgrad)


def solution(mesh):
    return jax.shard_map(
        local,
        mesh=mesh,
        in_specs=(
            P(("dom", "col"), None),
            P(),
            P(("dom", "col"), None),
            P(("dom", "col"), None, None),
            P(("dom", "col")),
            P(("dom", "col")),
            P(("dom", "col")),
            P(("dom", "col"), None),
        ),
        out_specs=(P(("dom", "col"), None), P(("dom", "col"), None), P()),
        check_vma=False,
    )
```
